32 devices in a mesh: eq: 2 (over x), row: 4 (over y, core), col: 4 (over z).
Axes of the slice: x: 2, y: 2, z: 4, core: 2. Of those that a mesh axis runs over, the one named last changes fastest.
Arguments:
- transition: float32 [6144, 3072], P(('eq', 'row'), 'col'), parts along dimension 0, may hold values from -0.05 to 0.9
- covariance: float32 [6144, 3072], P(('eq', 'row'), 'col'), parts along dimension 0, may hold values from -1 to 5, as said below
Outputs:
- covariance_out: float32 [6144, 3072], P(('eq', 'row'), 'col'), parts along dimension 0
- transition_out: float32 [6144, 3072], P(('eq', 'row'), 'col'), parts along dimension 0
The draws below stay inside these ranges and needn't reach their ends.
There are 2 independent parts, one for each index of `eq`. The reference program is written for one: setup_inputs(seed, part) draws one part's arguments, and reference() takes and returns one part's arrays. A program takes and returns all parts, laid end to end along the dimension named above; each array names one. Nothing has to cross between parts.
Inputs may be any that keep to these rules, and one draw needn't show every extreme that they name: covariance is exactly symmetric.
All inputs are finite; a program needn't handle non-finite values.
Results may differ from the reference program's by a relative error of at most 0.0001.
Values sent between devices are 32-bit elements; how exact they have to be, the bound alone decides.
A program may use at most 128 MiB of HBM per device.

```python
import jax
import jax.numpy as jnp
from jax import lax

ORDER = 3072
STEPS = 1


def draw_transition(key, part):
    keys = jax.random.split(jax.random.fold_in(key, 11), 2)
    diagonal = jax.random.uniform(keys[0], (ORDER,), jnp.float32, 0.5, 0.85)
    noise = jnp.clip(jax.random.normal(keys[1], (ORDER, ORDER), jnp.float32), -6.0, 6.0) * (0.12 / ORDER ** 0.5)
    noise = jnp.clip(noise, -0.05, 0.05)
    return noise + jnp.diag(diagonal)


def draw_covariance(key, part):
    keys = jax.random.split(jax.random.fold_in(key, 23), 3)
    diagonal = jax.random.uniform(keys[0], (ORDER,), jnp.float32, 1.0, 3.0)
    normals = jnp.clip(jax.random.normal(keys[1], (ORDER, ORDER), jnp.float32), -6.0, 6.0)
    noise = jnp.clip(normals * (0.4 / (2.0 * ORDER) ** 0.5), -0.45, 0.45)
    result = noise + noise.T + jnp.diag(diagonal)
    return result


def setup_inputs(seed: int = 0, part: int = 0) -> dict:
    key_list = jax.random.split(jax.random.key(seed), 3)
    part_splits = jax.random.split(jax.random.fold_in(key_list[2], part), 3)
    transition = draw_transition(jax.random.fold_in(jax.random.fold_in(key_list[2], part), 71), part)
    covariance = draw_covariance(jax.random.fold_in(jax.random.fold_in(key_list[2], part), 71), part)
    return dict(transition=transition, covariance=covariance)


def reference(transition, covariance):
    highest = lax.Precision.HIGHEST
    matrix = transition
    current = covariance
    for repeat in range(STEPS):
        product = jnp.dot(matrix, current, precision=highest, preferred_element_type=jnp.float32)
        current = jnp.dot(product, matrix.T, precision=highest, preferred_element_type=jnp.float32) + current
        matrix = jnp.dot(matrix, matrix, precision=highest, preferred_element_type=jnp.float32)
    return current, matrix
```

```python
import functools

import jax
import jax.numpy as jnp
from jax import lax
from jax.experimental import pallas as pl
from jax.experimental.pallas import tpu as pltpu
from jax.sharding import PartitionSpec as P

CHUNKS = 8
HALF = CHUNKS // 2
AHEAD = 2


def split(value):
    high = value.astype(jnp.bfloat16)
    return high, (value - high.astype(jnp.float32)).astype(jnp.bfloat16)


def product(stacked, high, low, transposed=False):
    dims = (((1,), (1 if transposed else 0,)), ((), ()))
    dot = functools.partial(lax.dot_general, dimension_numbers=dims, preferred_element_type=jnp.float32)
    step = stacked.shape[0] // 2
    both = dot(stacked, high)
    return both[:step] + (both[step:] + dot(stacked[:step], low))


def kernel(
    n, a_ref, x_ref, update_ref, square_ref,
    a_row, a_col, x_col, arrived, x_high, x_low, a_high, a_low, y_parts, lhs,
    local_sems, near_send, near_recv, far_send, far_recv, relay_send, relay_recv,
    gather_send, gather_recv, reduce_send, reduce_recv,
):
    r, z = lax.axis_index("row"), lax.axis_index("col")
    size = a_ref.shape[0]
    step = size // CHUNKS
    half_rows = size // 2
    last = n - 1
    pair = r // 2
    side = lax.rem(r, 2)
    far = lax.rem(r + n // 2, n)
    near = r + 1 - 2 * side
    far_near = lax.rem(near + n // 2, n)
    own_outer = jnp.where(pair == 0, 0, last)
    own_inner = jnp.where(pair == 0, 1, last - 1)
    far_outer = last - own_outer
    far_inner = last - own_inner
    at_end = (z == 0) | (z == last)
    inside = (z > 0) & (z < last)

    def rows(c):
        return pl.ds(pl.multiple_of(c * step, step), step)

    def loop(low, high, body):
        def one(i, carry):
            body(i)
            return carry

        lax.fori_loop(low, high, one, 0)

    def remote(src, dst, send, recv, **where):
        return pltpu.make_async_remote_copy(
            src_ref=src, dst_ref=dst, send_sem=send, recv_sem=recv,
            device_id=where, device_id_type=pl.DeviceIdType.MESH,
        )

    partial = x_col
    local = [
        pltpu.make_async_copy(a_ref, a_col.at[r], local_sems.at[0]),
        pltpu.make_async_copy(x_ref, x_col.at[r], local_sems.at[1]),
        pltpu.make_async_copy(x_ref, update_ref, local_sems.at[2]),
    ]
    for copy in local:
        copy.start()

    barrier = pltpu.get_barrier_semaphore()

    def greet(**where):
        pl.semaphore_signal(barrier, inc=1, device_id=where, device_id_type=pl.DeviceIdType.MESH)

    greet(row=far)
    greet(row=near)

    @pl.when(z > 0)
    def _():
        greet(col=z - 1)

    @pl.when(z < last)
    def _():
        greet(col=z + 1)

    pl.semaphore_wait(barrier, 4 - jnp.where(z == 0, 1, 0) - jnp.where(z == last, 1, 0))

    def gather_copy(right, hop, c):
        block = z - hop if right else z + hop
        slot = block if right else block - 1
        landing = a_row.at[slot, rows(c)]
        return remote(
            a_col.at[r, rows(c)] if hop == 0 else landing, landing,
            gather_send.at[0 if right else 1, hop, c], gather_recv.at[slot, c],
            col=z + 1 if right else z - 1,
        )

    def gather_arrival(block, c):
        slot = jnp.where(block > z, block - 1, block)
        remote(
            a_row.at[slot, rows(c)], a_row.at[slot, rows(c)],
            gather_send.at[0, 0, c], gather_recv.at[slot, c], row=near,
        ).wait_recv()

    def gather_own(c):
        @pl.when(z < last)
        def _():
            gather_copy(True, 0, c).start()

        @pl.when(z > 0)
        def _():
            gather_copy(False, 0, c).start()

    def pass_gather(right, hop, c):
        block = z - hop if right else z + hop
        valid = (block >= 0) if right else (block <= last)

        @pl.when(inside & valid)
        def _():
            gather_arrival(block, c)
            gather_copy(right, hop, c).start()

    def gather_slot(c):
        for hop in range(1, n - 1):
            pass_gather(True, hop, c)
            pass_gather(False, hop, c)

        @pl.when(inside & (c + AHEAD < CHUNKS))
        def _():
            gather_own(c + AHEAD)

    def gather_end(c):
        @pl.when(at_end)
        def _():
            for hop in range(1, n):
                gather_arrival(jnp.where(z == 0, hop, last - hop), c)

    def near_copy(which):
        buffer = (x_col, a_col)[which]
        return remote(buffer.at[r], buffer.at[r], near_send.at[which], near_recv.at[which], row=near)

    def near_wait(which):
        buffer = (x_col, a_col)[which]
        remote(buffer.at[near], buffer.at[near], near_send.at[which], near_recv.at[which], row=near).wait_recv()

    def half_of(piece, mine, rows_of):
        buffer = x_col if piece < 2 else a_col
        if piece < 2:
            block = (r, near)[piece] if mine else (far, far_near)[piece]
        else:
            block = ((own_outer, own_inner) if mine else (far_outer, far_inner))[piece - 2]
        return buffer.at[block, pl.ds(pl.multiple_of(rows_of * half_rows, half_rows), half_rows)]

    def far_copy(piece):
        ref = half_of(piece, True, side)
        return remote(ref, ref, far_send.at[piece], far_recv.at[piece], row=far)

    def relay_copy(piece):
        ref = half_of(piece, False, side)
        return remote(ref, ref, relay_send.at[piece], relay_recv.at[piece], row=near)

    def relay(piece):
        ref = half_of(piece, False, side)
        remote(ref, ref, far_send.at[piece], far_recv.at[piece], row=far).wait_recv()
        relay_copy(piece).start()

    def relay_wait(piece):
        ref = half_of(piece, False, 1 - side)
        remote(ref, ref, relay_send.at[piece], relay_recv.at[piece], row=near).wait_recv()

    def split_rows(which, block, low_row, count):
        source, high_ref, low_ref = ((x_col, x_high, x_low), (a_col, a_high, a_low))[which]

        def some(i):
            at = pl.multiple_of(low_row + i * step, step)
            high, low = split(source[block, pl.ds(at, step)])
            to = pl.ds(pl.multiple_of(block * size + at, step), step)
            high_ref[to] = high
            low_ref[to] = low

        loop(0, count // step, some)

    def split_half(which, block, which_half):
        split_rows(which, block, which_half * half_rows, half_rows)

    def multiply(c, high_ref, low_ref):
        for hop in range(n):
            block = lax.rem(z + hop, n)
            slot = jnp.where(block > z, block - 1, block)
            high, low = split(a_col[r, rows(c)] if hop == 0 else a_row[slot, rows(c)])
            to = pl.ds(pl.multiple_of(block * size, size), size)
            lhs[:step, to] = high
            lhs[step:, to] = low
        return product(lhs[...], high_ref[...], low_ref[...])

    def y_rows(c):
        return pl.ds(pl.multiple_of(lax.rem(c, HALF) * 2 * step, 2 * step), 2 * step)

    def compute_y(c):
        high, low = split(multiply(c, x_high, x_low))
        base = pl.multiple_of(lax.rem(c, HALF) * 2 * step, 2 * step)
        y_parts[pl.ds(base, step)] = high
        y_parts[pl.ds(pl.multiple_of(base + step, step), step)] = low

    def compute_square(c):
        square_ref[rows(c)] = multiply(c, a_high, a_low)

    def reduce_copy(right, d, c):
        target = jnp.where(right, z + 1, z - 1)
        slot = jnp.where(right & (d == target), n, d)
        return remote(
            partial.at[d, rows(c)], arrived.at[slot, rows(c)],
            reduce_send.at[d, c], reduce_recv.at[slot, c], col=target,
        )

    def reduce_wait(slot, c):
        remote(
            arrived.at[slot, rows(c)], arrived.at[slot, rows(c)],
            reduce_send.at[0, c], reduce_recv.at[slot, c], row=near,
        ).wait_recv()

    def compute_partial(c, d):
        block = pl.ds(pl.multiple_of(d * size, size), size)
        partial[d, rows(c)] = product(y_parts[y_rows(c)], a_high[block], a_low[block], transposed=True)

        @pl.when(((z == 0) & (d > 0)) | ((z == last) & (d < last)))
        def _():
            reduce_copy(z == 0, d, c).start()

    def early(c):
        gather_end(c)
        compute_y(c)
        loop(0, 2, lambda i: compute_partial(c, jnp.where(i == 0, own_outer, own_inner)))

    def late(c):
        gather_end(c)
        compute_y(c)
        loop(0, n, lambda i: compute_partial(c, jnp.where(z < n // 2, last - i, i)))

    def pass_piece(right, q):
        by_column = jnp.where(right, pair, 1 - pair) == 0
        first = q < CHUNKS
        outer = jnp.where(first & by_column, q // HALF, lax.rem(q, 2))
        c = jnp.where(first, jnp.where(by_column, lax.rem(q, HALF), q // 2), HALF + (q - CHUNKS) // 2)
        d = jnp.where(right, last - outer, outer)
        goes_on = jnp.where(right, d > z, d < z)

        @pl.when(inside & goes_on)
        def _():
            reduce_wait(d, c)
            partial[d, rows(c)] = partial[d, rows(c)] + arrived[d, rows(c)]
            reduce_copy(right, d, c).start()

    nearer_left = z < n // 2

    def first_hop(q):
        pass_piece(nearer_left, q)

    def second_hop(q):
        pass_piece(jnp.logical_not(nearer_left), q)

    local[0].wait()

    @pl.when(at_end)
    def _():
        loop(0, CHUNKS, gather_own)

    @pl.when(inside)
    def _():
        loop(0, AHEAD, gather_own)

    local[1].wait()
    far_copy(0).start()
    near_copy(0).start()
    near_copy(1).start()
    near_wait(0)
    far_copy(1).start()
    near_wait(1)
    far_copy(2).start()
    far_copy(3).start()

    def opening(c):
        gather_slot(c)

        @pl.when(c == 0)
        def _():
            split_rows(0, r, 0, size)
            split_rows(1, r, 0, size)

        @pl.when(c == 1)
        def _():
            relay(0)
            split_rows(0, near, 0, size)

        @pl.when(c == 2)
        def _():
            split_rows(1, near, 0, size)
            relay_wait(0)
            split_half(0, far, side)
            split_half(0, far_near, 1 - side)

    loop(0, HALF, opening)
    relay(1)
    split_half(0, far_near, side)
    relay_wait(1)
    split_half(0, far, 1 - side)
    near_copy(0).wait_send()
    for piece in range(2):
        far_copy(piece).wait_send()
        relay_copy(piece).wait_send()

    def second(c):
        gather_slot(HALF + c)
        early(c)

    loop(0, HALF - 1, second)
    relay(2)
    split_half(1, far_outer, side)
    relay_wait(2)
    split_half(1, far_outer, 1 - side)
    loop(0, HALF - 1, lambda c: compute_partial(c, far_outer))
    gather_slot(CHUNKS - 1)
    first_hop(0)
    first_hop(1)
    early(HALF - 1)
    compute_partial(HALF - 1, far_outer)
    first_hop(2)
    first_hop(3)
    relay(3)
    split_half(1, far_inner, side)
    relay_wait(3)
    split_half(1, far_inner, 1 - side)
    loop(0, HALF, lambda c: compute_partial(c, far_inner))

    def closing(j):
        for i in range(2):
            q = 4 + 2 * j + i

            @pl.when(q < 2 * CHUNKS)
            def _():
                first_hop(q)

        for i in range(2):
            second_hop(2 * j + i)

        @pl.when(j < HALF)
        def _():
            late(HALF + j)

        @pl.when((j >= 1) & (j <= HALF))
        def _():
            loop(2 * (j - 1), 2 * j, compute_square)

    loop(0, CHUNKS, closing)

    def finish(c):
        update_ref[rows(c)] = update_ref[rows(c)] + partial[z, rows(c)]

        @pl.when(z < last)
        def _():
            reduce_wait(z, c)
            update_ref[rows(c)] = update_ref[rows(c)] + arrived[z, rows(c)]

        @pl.when(z > 0)
        def _():
            reduce_wait(n, c)
            update_ref[rows(c)] = update_ref[rows(c)] + arrived[n, rows(c)]

    local[2].wait()
    loop(0, CHUNKS, finish)

    near_copy(1).wait_send()
    for piece in range(2, 4):
        far_copy(piece).wait_send()
        relay_copy(piece).wait_send()

    def sent(c):
        for hop in range(n - 1):
            @pl.when((z < last) & (z - hop >= 0))
            def _():
                gather_copy(True, hop, c).wait_send()

            @pl.when((z > 0) & (z + hop <= last))
            def _():
                gather_copy(False, hop, c).wait_send()

        for d in range(n):
            @pl.when(z != d)
            def _():
                reduce_copy(z < d, d, c).wait_send()

    loop(0, CHUNKS, sent)


def per_device(n, transition, covariance):
    size = transition.shape[0]
    f32, bf16 = jnp.float32, jnp.bfloat16
    shape = jax.ShapeDtypeStruct(transition.shape, f32)
    return pl.pallas_call(
        functools.partial(kernel, n),
        out_shape=(shape, shape),
        in_specs=[pl.BlockSpec(memory_space=pl.ANY)] * 2,
        out_specs=(pl.BlockSpec(memory_space=pltpu.VMEM),) * 2,
        scratch_shapes=[
            pltpu.VMEM((n - 1, size, size), f32),
            pltpu.VMEM((n, size, size), f32),
            pltpu.VMEM((n, size, size), f32),
            pltpu.VMEM((n + 1, size, size), f32),
            pltpu.VMEM((n * size, size), bf16),
            pltpu.VMEM((n * size, size), bf16),
            pltpu.VMEM((n * size, size), bf16),
            pltpu.VMEM((n * size, size), bf16),
            pltpu.VMEM((size, size), bf16),
            pltpu.VMEM((2 * size // CHUNKS, n * size), bf16),
            pltpu.SemaphoreType.DMA((3,)),
            pltpu.SemaphoreType.DMA((2,)),
            pltpu.SemaphoreType.DMA((2,)),
            pltpu.SemaphoreType.DMA((4,)),
            pltpu.SemaphoreType.DMA((4,)),
            pltpu.SemaphoreType.DMA((4,)),
            pltpu.SemaphoreType.DMA((4,)),
            pltpu.SemaphoreType.DMA((2, n - 1, CHUNKS)),
            pltpu.SemaphoreType.DMA((n - 1, CHUNKS)),
            pltpu.SemaphoreType.DMA((n, CHUNKS)),
            pltpu.SemaphoreType.DMA((n + 1, CHUNKS)),
        ],
        compiler_params=pltpu.CompilerParams(
            collective_id=0, has_side_effects=True, vmem_limit_bytes=67043328
        ),
    )(transition, covariance)


def solution(mesh):
    n = mesh.shape["col"]
    assert mesh.shape["row"] == n == 4
    spec = P(("eq", "row"), "col")
    return jax.shard_map(
        functools.partial(per_device, n),
        mesh=mesh,
        in_specs=(spec, spec),
        out_specs=(spec, spec),
        check_vma=False,
    )
```

```python
import functools

import jax
import jax.numpy as jnp
from jax import lax
from jax.experimental import pallas as pl
from jax.experimental.pallas import tpu as pltpu
from jax.sharding import PartitionSpec as P

CHUNKS = 8
AHEAD = 2
ORDERS = (
  (
    253789560, 33963514, 38176921, 245107104, 42500513, 44483107, 24132337, 154166277,
    155554370, 157388355, 26486340, 173296626, 79196278, 211349767, 145189459, 28190437,
    241802453, 187608183, 194440478, 30514653, 127119206, 65803222, 167244743, 219535503,
    223122537, 227333355, 231544173, 111861487, 113991468, 99475374,
  ),
  (
    253789560, 33963514, 38176921, 245107104, 42500513, 44483107, 24132337, 137768965,
    187011681, 60207426, 192471430, 144477068, 78799990, 210953479, 117925468, 28799685,
    120170160, 171195379, 215062686, 121874270, 179644882, 65835990, 200926139, 183289807,
    126498024, 109737450, 128628460, 111867886, 113991468, 99473215,
  ),
  (
    259964152, 247233136, 170944576, 154282306, 175940042, 205011787, 210842082, 186513868,
    194440537, 163017413, 165131078, 219673543, 228259177, 167507821, 183872212, 268435455,
    268435455, 268435455, 268435455, 268435455, 268435455, 268435455, 268435455, 268435455,
    268435455, 268435455, 268435455, 268435455, 268435455, 268435455,
  ),
  (
    259964152, 247233136, 137769024, 206613729, 209494490, 154286939, 210838986, 251455068,
    196700229, 215245645, 173139806, 221917159, 230372842, 167504366, 183872212, 268435455,
    268435455, 268435455, 268435455, 268435455, 268435455, 268435455, 268435455, 268435455,
    268435455, 268435455, 268435455, 268435455, 268435455, 268435455,
  ),
)


def split(value):
    high = value.astype(jnp.bfloat16)
    return high, (value - high.astype(jnp.float32)).astype(jnp.bfloat16)


def product(stacked, high, low, transposed=False):
    dims = (((1,), (1 if transposed else 0,)), ((), ()))
    dot = functools.partial(lax.dot_general, dimension_numbers=dims, preferred_element_type=jnp.float32)
    step = stacked.shape[0] // 2
    both = dot(stacked, high)
    return both[:step] + (both[step:] + dot(stacked[:step], low))


def kernel(
    n, a_ref, x_ref, update_ref, square_ref,
    a_row, a_col, x_col, arrived, x_high, x_low, a_high, a_low, y_parts, lhs,
    local_sems, near_send, near_recv, far_send, far_recv, relay_send, relay_recv,
    gather_send, gather_recv, reduce_send, reduce_recv,
):
    r, z = lax.axis_index("row"), lax.axis_index("col")
    size = a_ref.shape[0]
    step = size // CHUNKS
    half_rows = size // 2
    last = n - 1
    pair = r // 2
    side = lax.rem(r, 2)
    far = lax.rem(r + n // 2, n)
    near = r + 1 - 2 * side
    far_near = lax.rem(near + n // 2, n)
    own_outer = jnp.where(pair == 0, 0, last)
    own_inner = jnp.where(pair == 0, 1, last - 1)
    far_outer = last - own_outer
    far_inner = last - own_inner
    at_end = (z == 0) | (z == last)
    inside = (z > 0) & (z < last)

    def rows(c):
        return pl.ds(pl.multiple_of(c * step, step), step)

    def loop(low, high, body):
        def one(i, carry):
            body(i)
            return carry

        lax.fori_loop(low, high, one, 0)

    def remote(src, dst, send, recv, **where):
        return pltpu.make_async_remote_copy(
            src_ref=src, dst_ref=dst, send_sem=send, recv_sem=recv,
            device_id=where, device_id_type=pl.DeviceIdType.MESH,
        )

    partial = x_col
    local = [
        pltpu.make_async_copy(a_ref, a_col.at[r], local_sems.at[0]),
        pltpu.make_async_copy(x_ref, x_col.at[r], local_sems.at[1]),
        pltpu.make_async_copy(x_ref, update_ref, local_sems.at[2]),
    ]
    for copy in local:
        copy.start()

    barrier = pltpu.get_barrier_semaphore()

    def greet(**where):
        pl.semaphore_signal(barrier, inc=1, device_id=where, device_id_type=pl.DeviceIdType.MESH)

    greet(row=far)
    greet(row=near)

    @pl.when(z > 0)
    def _():
        greet(col=z - 1)

    @pl.when(z < last)
    def _():
        greet(col=z + 1)

    pl.semaphore_wait(barrier, 4 - jnp.where(z == 0, 1, 0) - jnp.where(z == last, 1, 0))

    def gather_copy(right, block, c):
        slot = jnp.where(right, block, block - 1)
        landing = a_row.at[slot, rows(c)]
        sems = gather_send.at[jnp.where(right, 0, 1), jnp.abs(block - z), c], gather_recv.at[slot, c]
        to = jnp.where(right, z + 1, z - 1)
        return landing, sems, to

    def gather_own(right, c):
        landing, sems, to = gather_copy(right, z, c)
        return remote(a_col.at[r, rows(c)], landing, *sems, col=to)

    def gather_pass(right, block, c):
        landing, sems, to = gather_copy(right, block, c)
        return remote(landing, landing, *sems, col=to)

    def gather_arrival(block, c):
        slot = jnp.where(block > z, block - 1, block)
        remote(
            a_row.at[slot, rows(c)], a_row.at[slot, rows(c)],
            gather_send.at[0, 0, c], gather_recv.at[slot, c], row=near,
        ).wait_recv()

    def own_both(c):
        @pl.when(z < last)
        def _():
            gather_own(True, c).start()

        @pl.when(z > 0)
        def _():
            gather_own(False, c).start()

    def pass_gather(block, c):
        gather_arrival(block, c)
        gather_pass(block < z, block, c).start()

    def gather_end(c):
        @pl.when(at_end)
        def _():
            for hop in range(1, n):
                gather_arrival(jnp.where(z == 0, hop, last - hop), c)

    def near_copy(which):
        buffer = (x_col, a_col)[which]
        return remote(buffer.at[r], buffer.at[r], near_send.at[which], near_recv.at[which], row=near)

    def near_wait(which):
        buffer = (x_col, a_col)[which]
        remote(buffer.at[near], buffer.at[near], near_send.at[which], near_recv.at[which], row=near).wait_recv()

    def half_of(piece, mine, rows_of):
        buffer = x_col if piece < 2 else a_col
        if piece < 2:
            block = (r, near)[piece] if mine else (far, far_near)[piece]
        else:
            block = ((own_outer, own_inner) if mine else (far_outer, far_inner))[piece - 2]
        return buffer.at[block, pl.ds(pl.multiple_of(rows_of * half_rows, half_rows), half_rows)]

    def far_copy(piece):
        ref = half_of(piece, True, side)
        return remote(ref, ref, far_send.at[piece], far_recv.at[piece], row=far)

    def relay_copy(piece):
        ref = half_of(piece, False, side)
        return remote(ref, ref, relay_send.at[piece], relay_recv.at[piece], row=near)

    def relay(piece):
        ref = half_of(piece, False, side)
        remote(ref, ref, far_send.at[piece], far_recv.at[piece], row=far).wait_recv()
        relay_copy(piece).start()

    def relay_wait(piece):
        ref = half_of(piece, False, 1 - side)
        remote(ref, ref, relay_send.at[piece], relay_recv.at[piece], row=near).wait_recv()

    def split_rows(which, block, low_row, count):
        source, high_ref, low_ref = ((x_col, x_high, x_low), (a_col, a_high, a_low))[which]

        def some(i):
            at = pl.multiple_of(low_row + i * step, step)
            high, low = split(source[block, pl.ds(at, step)])
            to = pl.ds(pl.multiple_of(block * size + at, step), step)
            high_ref[to] = high
            low_ref[to] = low

        loop(0, count // step, some)

    def split_half(which, block, which_half):
        split_rows(which, block, which_half * half_rows, half_rows)

    def multiply(c, high_ref, low_ref):
        for hop in range(n):
            block = lax.rem(z + hop, n)
            slot = jnp.where(block > z, block - 1, block)
            high, low = split(a_col[r, rows(c)] if hop == 0 else a_row[slot, rows(c)])
            to = pl.ds(pl.multiple_of(block * size, size), size)
            lhs[:step, to] = high
            lhs[step:, to] = low
        return product(lhs[...], high_ref[...], low_ref[...])

    def y_rows(c):
        return pl.ds(pl.multiple_of(c * 2 * step, 2 * step), 2 * step)

    def compute_y(c):
        high, low = split(multiply(c, x_high, x_low))
        base = pl.multiple_of(c * 2 * step, 2 * step)
        y_parts[pl.ds(base, step)] = high
        y_parts[pl.ds(pl.multiple_of(base + step, step), step)] = low

    def compute_square(c):
        square_ref[rows(c)] = multiply(c, a_high, a_low)

    def reduce_copy(right, d, c):
        target = jnp.where(right, z + 1, z - 1)
        slot = jnp.where(right & (d == target), n, d)
        return remote(
            partial.at[d, rows(c)], arrived.at[slot, rows(c)],
            reduce_send.at[d, c], reduce_recv.at[slot, c], col=target,
        )

    def reduce_wait(slot, c):
        remote(
            arrived.at[slot, rows(c)], arrived.at[slot, rows(c)],
            reduce_send.at[0, c], reduce_recv.at[slot, c], row=near,
        ).wait_recv()

    def compute_partial(c, d):
        block = pl.ds(pl.multiple_of(d * size, size), size)
        partial[d, rows(c)] = product(y_parts[y_rows(c)], a_high[block], a_low[block], transposed=True)

        @pl.when(((z == 0) & (d > 0)) | ((z == last) & (d < last)))
        def _():
            reduce_copy(z == 0, d, c).start()

    def pass_piece(d, c):
        reduce_wait(d, c)
        partial[d, rows(c)] = partial[d, rows(c)] + arrived[d, rows(c)]
        reduce_copy(d > z, d, c).start()

    def landed(piece):
        relay_wait(piece)
        if piece < 2:
            split_half(0, (far, far_near)[piece], side)
            split_half(0, (far_near, far)[piece], 1 - side)
        else:
            split_rows(1, (far_outer, far_inner)[piece - 2], 0, size)
        if piece == 1:
            near_copy(0).wait_send()
            for sent_piece in range(2):
                far_copy(sent_piece).wait_send()
                relay_copy(sent_piece).wait_send()

    mirrored = z >= n // 2

    def facing(index):
        return jnp.where(mirrored, last - index, index)

    def other(index):
        return facing(jnp.where(index >= 1, index + 1, index))

    def act(code):
        def when(low, count, body):
            @pl.when((code >= low) & (code < low + count))
            def _():
                body((code - low) // CHUNKS, lax.rem(code - low, CHUNKS))

        def once(value, body):
            @pl.when(code == value)
            def _():
                body()

        when(0, 2 * CHUNKS, lambda i, c: gather_own((i == 0) != mirrored, c).start())
        when(16, 3 * CHUNKS, lambda i, c: pass_gather(other(i), c))
        when(40, 3 * CHUNKS, lambda i, c: pass_piece(other(i), c))

        def begin(i, c):
            gather_end(c)
            compute_y(c)

        when(64, CHUNKS, begin)
        when(72, 4 * CHUNKS, lambda i, c: compute_partial(c, facing(i)))
        when(104, CHUNKS, lambda i, c: compute_square(c))
        for piece in range(4):
            once(112 + piece, functools.partial(relay, piece))
            once(116 + piece, functools.partial(landed, piece))
        once(120, lambda: split_rows(0, r, 0, size))
        once(121, lambda: split_rows(0, near, 0, size))
        once(122, lambda: split_rows(1, r, 0, size))
        once(123, lambda: split_rows(1, near, 0, size))

    local[0].wait()

    @pl.when(at_end)
    def _():
        loop(0, CHUNKS, own_both)

    @pl.when(inside)
    def _():
        loop(0, AHEAD, own_both)

    local[1].wait()
    far_copy(0).start()
    near_copy(0).start()
    near_copy(1).start()
    near_wait(0)
    far_copy(1).start()
    near_wait(1)
    far_copy(2).start()
    far_copy(3).start()

    second = (pair == 0) == mirrored
    choice = jnp.where(at_end, 2, 0) + jnp.where(second, 1, 0)

    def four(i):
        word = 0
        for at in range(len(ORDERS[0])):
            value = ORDERS[3][at]
            for v in range(3):
                value = jnp.where(choice == v, ORDERS[v][at], value)
            word = jnp.where(i == at, value, word)

        def one(j, left):
            act(lax.rem(left, 128))
            return left // 128

        lax.fori_loop(0, 4, one, word)

    loop(0, len(ORDERS[0]), four)

    def finish(c):
        update_ref[rows(c)] = update_ref[rows(c)] + partial[z, rows(c)]

        @pl.when(z < last)
        def _():
            reduce_wait(z, c)
            update_ref[rows(c)] = update_ref[rows(c)] + arrived[z, rows(c)]

        @pl.when(z > 0)
        def _():
            reduce_wait(n, c)
            update_ref[rows(c)] = update_ref[rows(c)] + arrived[n, rows(c)]

    local[2].wait()
    loop(0, CHUNKS, finish)

    near_copy(1).wait_send()
    for piece in range(2, 4):
        far_copy(piece).wait_send()
        relay_copy(piece).wait_send()

    def sent(c):
        for hop in range(n - 1):
            @pl.when((z < last) & (z - hop >= 0))
            def _():
                gather_pass(True, z - hop, c).wait_send()

            @pl.when((z > 0) & (z + hop <= last))
            def _():
                gather_pass(False, z + hop, c).wait_send()

        for d in range(n):
            @pl.when(z != d)
            def _():
                reduce_copy(z < d, d, c).wait_send()

    loop(0, CHUNKS, sent)


def per_device(n, transition, covariance):
    size = transition.shape[0]
    f32, bf16 = jnp.float32, jnp.bfloat16
    shape = jax.ShapeDtypeStruct(transition.shape, f32)
    return pl.pallas_call(
        functools.partial(kernel, n),
        out_shape=(shape, shape),
        in_specs=[pl.BlockSpec(memory_space=pl.ANY)] * 2,
        out_specs=(pl.BlockSpec(memory_space=pltpu.VMEM),) * 2,
        scratch_shapes=[
            pltpu.VMEM((n - 1, size, size), f32),
            pltpu.VMEM((n, size, size), f32),
            pltpu.VMEM((n, size, size), f32),
            pltpu.VMEM((n + 1, size, size), f32),
            pltpu.VMEM((n * size, size), bf16),
            pltpu.VMEM((n * size, size), bf16),
            pltpu.VMEM((n * size, size), bf16),
            pltpu.VMEM((n * size, size), bf16),
            pltpu.VMEM((2 * size, size), bf16),
            pltpu.VMEM((2 * size // CHUNKS, n * size), bf16),
            pltpu.SemaphoreType.DMA((3,)),
            pltpu.SemaphoreType.DMA((2,)),
            pltpu.SemaphoreType.DMA((2,)),
            pltpu.SemaphoreType.DMA((4,)),
            pltpu.SemaphoreType.DMA((4,)),
            pltpu.SemaphoreType.DMA((4,)),
            pltpu.SemaphoreType.DMA((4,)),
            pltpu.SemaphoreType.DMA((2, n - 1, CHUNKS)),
            pltpu.SemaphoreType.DMA((n - 1, CHUNKS)),
            pltpu.SemaphoreType.DMA((n, CHUNKS)),
            pltpu.SemaphoreType.DMA((n + 1, CHUNKS)),
        ],
        compiler_params=pltpu.CompilerParams(
            collective_id=0, has_side_effects=True, vmem_limit_bytes=67043328
        ),
    )(transition, covariance)


def solution(mesh):
    n = mesh.shape["col"]
    assert mesh.shape["row"] == n == 4
    spec = P(("eq", "row"), "col")
    return jax.shard_map(
        functools.partial(per_device, n),
        mesh=mesh,
        in_specs=(spec, spec),
        out_specs=(spec, spec),
        check_vma=False,
    )
```

```python
import functools

import jax
import jax.numpy as jnp
from jax import lax
from jax.experimental import pallas as pl
from jax.experimental.pallas import tpu as pltpu
from jax.sharding import PartitionSpec as P

CHUNKS = 8
AHEAD = 2
LATE = 1
ORDERS = (
  (
    255721738, 6686731, 38176921, 40303216, 8931872, 247220898, 152044195, 153457217,
    13051202, 26289603, 240395799, 15296849, 207122550, 146345699, 174286565, 81095224,
    64879033, 190209368, 196544347, 83469115, 181348190, 256648095, 32763879, 221911255,
    225228072, 229439017, 233649962, 111877803, 258842413, 100630318,
  ),
  (
    255721738, 6686731, 38176921, 40303216, 8931872, 247220898, 202375843, 136680024,
    59813089, 141996294, 192465804, 15295090, 156394614, 210636491, 28403292, 163017392,
    251452582, 171186334, 214861638, 175417182, 179640615, 149868502, 167244794, 219535759,
    223286377, 227349739, 231691629, 93148655, 258693950, 100630318,
  ),
  (
    245120248, 168835825, 154427592, 141732162, 248703474, 209236192, 242430532, 190213239,
    212954715, 215066333, 219277150, 228259177, 177993581, 267758287, 268435455, 268435455,
    268435455, 268435455, 268435455, 268435455, 268435455, 268435455, 268435455, 268435455,
    268435455, 268435455, 268435455, 268435455, 268435455, 268435455,
  ),
  (
    245120248, 202390257, 188244184, 141996354, 248967666, 158508232, 160903748, 212958195,
    148121309, 171159398, 224031815, 175846866, 234174317, 267758287, 268435455, 268435455,
    268435455, 268435455, 268435455, 268435455, 268435455, 268435455, 268435455, 268435455,
    268435455, 268435455, 268435455, 268435455, 268435455, 268435455,
  ),
)


def split(value):
    high = value.astype(jnp.bfloat16)
    return high, (value - high.astype(jnp.float32)).astype(jnp.bfloat16)


def product(stacked, high, low, transposed=False):
    dims = (((1,), (1 if transposed else 0,)), ((), ()))
    dot = functools.partial(lax.dot_general, dimension_numbers=dims, preferred_element_type=jnp.float32)
    step = stacked.shape[0] // 2
    both = dot(stacked, high)
    return both[:step] + (both[step:] + dot(stacked[:step], low))


def kernel(
    n, a_ref, x_ref, update_ref, square_ref,
    a_row, a_col, x_col, arrived, x_high, x_low, a_high, a_low, y_parts, lhs,
    local_sems, near_send, near_recv, far_send, far_recv, relay_send, relay_recv,
    gather_send, gather_recv, reduce_send, reduce_recv, end_send, end_recv, free_sems,
):
    r, z = lax.axis_index("row"), lax.axis_index("col")
    size = a_ref.shape[0]
    step = size // CHUNKS
    half_rows = size // 2
    last = n - 1
    pair = r // 2
    side = lax.rem(r, 2)
    far = lax.rem(r + n // 2, n)
    near = r + 1 - 2 * side
    far_near = lax.rem(near + n // 2, n)
    own_outer = jnp.where(pair == 0, 0, last)
    own_inner = jnp.where(pair == 0, 1, last - 1)
    far_outer = last - own_outer
    far_inner = last - own_inner
    at_end = (z == 0) | (z == last)
    inside = (z > 0) & (z < last)
    beside = jnp.where(z == 0, 1, last - 1)

    def rows(c):
        return pl.ds(pl.multiple_of(c * step, step), step)

    def loop(low, high, body):
        def one(i, carry):
            body(i)
            return carry

        lax.fori_loop(low, high, one, 0)

    def remote(src, dst, send, recv, **where):
        return pltpu.make_async_remote_copy(
            src_ref=src, dst_ref=dst, send_sem=send, recv_sem=recv,
            device_id=where, device_id_type=pl.DeviceIdType.MESH,
        )

    partial = x_col
    local = [
        pltpu.make_async_copy(a_ref, a_col.at[r], local_sems.at[0]),
        pltpu.make_async_copy(x_ref, x_col.at[r], local_sems.at[1]),
        pltpu.make_async_copy(x_ref, update_ref, local_sems.at[2]),
    ]
    for copy in local:
        copy.start()

    barrier = pltpu.get_barrier_semaphore()

    def greet(**where):
        pl.semaphore_signal(barrier, inc=1, device_id=where, device_id_type=pl.DeviceIdType.MESH)

    greet(row=far)
    greet(row=near)

    @pl.when(z > 0)
    def _():
        greet(col=z - 1)

    @pl.when(z < last)
    def _():
        greet(col=z + 1)

    pl.semaphore_wait(barrier, 4 - jnp.where(z == 0, 1, 0) - jnp.where(z == last, 1, 0))

    def gather_copy(right, block, c):
        slot = jnp.where(right, block, block - 1)
        landing = a_row.at[slot, rows(c)]
        sems = gather_send.at[jnp.where(right, 0, 1), jnp.abs(block - z), c], gather_recv.at[slot, c]
        to = jnp.where(right, z + 1, z - 1)
        return landing, sems, to

    def gather_own(right, c):
        landing, sems, to = gather_copy(right, z, c)
        return remote(a_col.at[r, rows(c)], landing, *sems, col=to)

    def gather_pass(right, block, c):
        landing, sems, to = gather_copy(right, block, c)
        return remote(landing, landing, *sems, col=to)

    def gather_arrival(block, c):
        slot = jnp.where(block > z, block - 1, block)
        remote(
            a_row.at[slot, rows(c)], a_row.at[slot, rows(c)],
            gather_send.at[0, 0, c], gather_recv.at[slot, c], row=near,
        ).wait_recv()

    def own_both(c):
        @pl.when(z < last)
        def _():
            gather_own(True, c).start()

        @pl.when(z > 0)
        def _():
            gather_own(False, c).start()

    def pass_gather(block, c):
        gather_arrival(block, c)
        gather_pass(block < z, block, c).start()

    def gather_end(c):
        @pl.when(at_end)
        def _():
            for hop in range(1, n):
                gather_arrival(jnp.where(z == 0, hop, last - hop), c)

    def near_copy(which):
        buffer = (x_col, a_col)[which]
        return remote(buffer.at[r], buffer.at[r], near_send.at[which], near_recv.at[which], row=near)

    def near_wait(which):
        buffer = (x_col, a_col)[which]
        remote(buffer.at[near], buffer.at[near], near_send.at[which], near_recv.at[which], row=near).wait_recv()

    def half_of(piece, mine, rows_of):
        buffer = x_col if piece < 2 else a_col
        if piece < 2:
            block = (r, near)[piece] if mine else (far, far_near)[piece]
        else:
            block = ((own_outer, own_inner) if mine else (far_outer, far_inner))[piece - 2]
        return buffer.at[block, pl.ds(pl.multiple_of(rows_of * half_rows, half_rows), half_rows)]

    def far_copy(piece):
        ref = half_of(piece, True, side)
        return remote(ref, ref, far_send.at[piece], far_recv.at[piece], row=far)

    def relay_copy(piece):
        ref = half_of(piece, False, side)
        return remote(ref, ref, relay_send.at[piece], relay_recv.at[piece], row=near)

    def relay(piece):
        ref = half_of(piece, False, side)
        remote(ref, ref, far_send.at[piece], far_recv.at[piece], row=far).wait_recv()
        relay_copy(piece).start()

    def relay_wait(piece):
        ref = half_of(piece, False, 1 - side)
        remote(ref, ref, relay_send.at[piece], relay_recv.at[piece], row=near).wait_recv()

    x_pair, a_pair = (x_high, x_low), (a_high, a_low)

    def split_rows(source, pair_refs, block, low_row, count):
        def some(i):
            at = pl.multiple_of(low_row + i * step, step)
            to = pl.ds(pl.multiple_of(block * size + at, step), step)
            pair_refs[0][to], pair_refs[1][to] = split(source[pl.ds(at, step)])

        loop(0, count // step, some)

    def split_half(block, which_half):
        split_rows(x_col.at[block], x_pair, block, which_half * half_rows, half_rows)

    def split_all(source, pair_refs, block):
        split_rows(source, pair_refs, block, 0, size)

    def multiply(c, high_ref, low_ref):
        for hop in range(n):
            block = lax.rem(z + hop, n)
            slot = jnp.where(block > z, block - 1, block)
            high, low = split(a_col[r, rows(c)] if hop == 0 else a_row[slot, rows(c)])
            to = pl.ds(pl.multiple_of(block * size, size), size)
            lhs[:step, to] = high
            lhs[step:, to] = low
        return product(lhs[...], high_ref[...], low_ref[...])

    def y_rows(c):
        return pl.ds(pl.multiple_of(c * 2 * step, 2 * step), 2 * step)

    def compute_y(c):
        value = multiply(c, x_high, x_low)

        @pl.when(at_end & (c >= CHUNKS - LATE))
        def _():
            partial[beside, rows(c)] = value

        high, low = split(value)
        base = pl.multiple_of(c * 2 * step, 2 * step)
        y_parts[pl.ds(base, step)] = high
        y_parts[pl.ds(pl.multiple_of(base + step, step), step)] = low

    def compute_square(c):
        square_ref[rows(c)] = multiply(c, a_high, a_low)

    def reduce_copy(right, d, c):
        target = jnp.where(right, z + 1, z - 1)
        slot = jnp.where(right & (d == target), n, d)
        return remote(
            partial.at[d, rows(c)], arrived.at[slot, rows(c)],
            reduce_send.at[d, c], reduce_recv.at[slot, c], col=target,
        )

    def reduce_wait(slot, c):
        remote(
            arrived.at[slot, rows(c)], arrived.at[slot, rows(c)],
            reduce_send.at[0, c], reduce_recv.at[slot, c], row=near,
        ).wait_recv()

    def compute_partial(c, d):
        block = pl.ds(pl.multiple_of(d * size, size), size)
        partial[d, rows(c)] = product(y_parts[y_rows(c)], a_high[block], a_low[block], transposed=True)

        @pl.when(((z == 0) & (d > 0)) | ((z == last) & (d < last)))
        def _():
            reduce_copy(z == 0, d, c).start()

    def pass_piece(d, c):
        reduce_wait(d, c)
        partial[d, rows(c)] = partial[d, rows(c)] + arrived[d, rows(c)]
        reduce_copy(d > z, d, c).start()

    def landed(piece):
        relay_wait(piece)
        if piece < 2:
            split_half((far, far_near)[piece], side)
            split_half((far_near, far)[piece], 1 - side)
        else:
            block = (far_outer, far_inner)[piece - 2]
            split_all(a_col.at[block], a_pair, block)
        if piece == 1:
            near_copy(0).wait_send()
            for sent_piece in range(2):
                far_copy(sent_piece).wait_send()
                relay_copy(sent_piece).wait_send()
        if piece == 3:
            for sent_piece in range(2, 4):
                far_copy(sent_piece).wait_send()
                relay_copy(sent_piece).wait_send()

            @pl.when(inside)
            def _():
                for at, row in ((0, near), (1, far)):
                    pl.semaphore_signal(
                        free_sems.at[at], inc=1, device_id={"row": row}, device_id_type=pl.DeviceIdType.MESH
                    )

    mirrored = z >= n // 2
    end_slot = jnp.where(mirrored, n - 2, 0)

    def end_copy(which):
        source, block, row = (
            (a_row.at[end_slot], r, far), (a_row.at[end_slot], r, near), (a_col.at[far], far, near)
        )[which]
        return remote(source, a_col.at[block], end_send.at[which], end_recv.at[which], row=row)

    def end_wait(which):
        block = (far, near, far_near)[which]
        remote(a_col.at[block], a_col.at[block], end_send.at[which], end_recv.at[which], row=near).wait_recv()

    def end_start():
        pl.semaphore_wait(free_sems.at[0], 1)
        pl.semaphore_wait(free_sems.at[1], 1)
        end_copy(0).start()
        end_copy(1).start()

    def end_middle():
        end_wait(0)
        end_copy(2).start()
        split_all(a_row.at[end_slot], x_pair, r)
        end_wait(1)
        split_all(a_col.at[near], x_pair, near)
        split_all(a_col.at[far], x_pair, far)

    def end_last():
        end_wait(2)
        split_all(a_col.at[far_near], x_pair, far_near)

    def end_partials(c):
        slot = jnp.where(mirrored, z, n)
        reduce_wait(slot, c)
        high, low = split(arrived[slot, rows(c)])
        lhs[:step, :size] = high
        lhs[step:, :size] = low

        def one(i):
            d = jnp.where(mirrored, i, last - i)
            block = pl.ds(pl.multiple_of(d * size, size), size)
            partial[d, rows(c)] = partial[d, rows(c)] + product(
                lhs[:, :size], x_high[block], x_low[block], transposed=True
            )

            @pl.when(i < n // 2)
            def _():
                reduce_copy(d > z, d, c).start()

        loop(0, n - 1, one)

    def facing(index):
        return jnp.where(mirrored, last - index, index)

    def other(index):
        return facing(jnp.where(index >= 1, index + 1, index))

    def act(code):
        def when(low, count, body):
            @pl.when((code >= low) & (code < low + count))
            def _():
                body((code - low) // CHUNKS, lax.rem(code - low, CHUNKS))

        def once(value, body):
            @pl.when(code == value)
            def _():
                body()

        when(0, 2 * CHUNKS, lambda i, c: gather_own((i == 0) != mirrored, c).start())
        when(16, 3 * CHUNKS, lambda i, c: pass_gather(other(i), c))
        when(40, 3 * CHUNKS, lambda i, c: pass_piece(other(i), c))

        def begin(i, c):
            gather_end(c)
            compute_y(c)

            @pl.when(at_end & (c >= CHUNKS - LATE))
            def _():
                reduce_copy(z == 0, beside, c).start()

        when(64, CHUNKS, begin)
        when(72, 4 * CHUNKS, lambda i, c: compute_partial(c, facing(i)))
        when(104, CHUNKS, lambda i, c: compute_square(c))
        for piece in range(4):
            once(112 + piece, functools.partial(relay, piece))
            once(116 + piece, functools.partial(landed, piece))
        once(120, lambda: split_both(x_col, x_pair))
        once(121, lambda: split_both(a_col, a_pair))
        once(122, end_start)
        once(123, end_middle)
        once(126, end_last)
        once(125, lambda: end_partials(CHUNKS - 1))

    def split_both(source, pair_refs):
        def one(i):
            block = jnp.where(i == 0, r, near)
            split_all(source.at[block], pair_refs, block)

        loop(0, 2, one)

    local[1].wait()
    far_copy(0).start()
    near_copy(0).start()
    local[0].wait()

    @pl.when(at_end)
    def _():
        loop(0, CHUNKS, own_both)

    @pl.when(inside)
    def _():
        loop(0, AHEAD, own_both)

    near_copy(1).start()
    near_wait(0)
    far_copy(1).start()
    near_wait(1)
    far_copy(2).start()
    far_copy(3).start()

    second = (pair == 0) == mirrored
    choice = jnp.where(at_end, 2, 0) + jnp.where(second, 1, 0)

    def four(i):
        word = 0
        for at in range(len(ORDERS[0])):
            value = ORDERS[3][at]
            for v in range(3):
                value = jnp.where(choice == v, ORDERS[v][at], value)
            word = jnp.where(i == at, value, word)

        def one(j, left):
            act(lax.rem(left, 128))
            return left // 128

        lax.fori_loop(0, 4, one, word)

    loop(0, len(ORDERS[0]), four)

    def finish(c):
        update_ref[rows(c)] = update_ref[rows(c)] + partial[z, rows(c)]

        early = c < CHUNKS - LATE

        @pl.when((z < last) & (early | (z != last - 1)))
        def _():
            reduce_wait(z, c)
            update_ref[rows(c)] = update_ref[rows(c)] + arrived[z, rows(c)]

        @pl.when((z > 0) & (early | (z != 1)))
        def _():
            reduce_wait(n, c)
            update_ref[rows(c)] = update_ref[rows(c)] + arrived[n, rows(c)]

    local[2].wait()
    loop(0, CHUNKS, finish)

    near_copy(1).wait_send()

    @pl.when(inside)
    def _():
        for which in range(3):
            end_copy(which).wait_send()

    def sent(c):
        for hop in range(n - 1):
            @pl.when((z < last) & (z - hop >= 0))
            def _():
                gather_pass(True, z - hop, c).wait_send()

            @pl.when((z > 0) & (z + hop <= last))
            def _():
                gather_pass(False, z + hop, c).wait_send()

        for d in range(n):
            @pl.when((z != d) & (inside | (c < CHUNKS - LATE) | (d == beside)))
            def _():
                reduce_copy(z < d, d, c).wait_send()

    loop(0, CHUNKS, sent)


def per_device(n, transition, covariance):
    size = transition.shape[0]
    f32, bf16 = jnp.float32, jnp.bfloat16
    shape = jax.ShapeDtypeStruct(transition.shape, f32)
    return pl.pallas_call(
        functools.partial(kernel, n),
        out_shape=(shape, shape),
        in_specs=[pl.BlockSpec(memory_space=pl.ANY)] * 2,
        out_specs=(pl.BlockSpec(memory_space=pltpu.VMEM),) * 2,
        scratch_shapes=[
            pltpu.VMEM((n - 1, size, size), f32),
            pltpu.VMEM((n, size, size), f32),
            pltpu.VMEM((n, size, size), f32),
            pltpu.VMEM((n + 1, size, size), f32),
            pltpu.VMEM((n * size, size), bf16),
            pltpu.VMEM((n * size, size), bf16),
            pltpu.VMEM((n * size, size), bf16),
            pltpu.VMEM((n * size, size), bf16),
            pltpu.VMEM((2 * size, size), bf16),
            pltpu.VMEM((2 * size // CHUNKS, n * size), bf16),
            pltpu.SemaphoreType.DMA((3,)),
            pltpu.SemaphoreType.DMA((2,)),
            pltpu.SemaphoreType.DMA((2,)),
            pltpu.SemaphoreType.DMA((4,)),
            pltpu.SemaphoreType.DMA((4,)),
            pltpu.SemaphoreType.DMA((4,)),
            pltpu.SemaphoreType.DMA((4,)),
            pltpu.SemaphoreType.DMA((2, n - 1, CHUNKS)),
            pltpu.SemaphoreType.DMA((n - 1, CHUNKS)),
            pltpu.SemaphoreType.DMA((n, CHUNKS)),
            pltpu.SemaphoreType.DMA((n + 1, CHUNKS)),
            pltpu.SemaphoreType.DMA((3,)),
            pltpu.SemaphoreType.DMA((3,)),
            pltpu.SemaphoreType.REGULAR((2,)),
        ],
        compiler_params=pltpu.CompilerParams(
            collective_id=0, has_side_effects=True, vmem_limit_bytes=67043328
        ),
    )(transition, covariance)


def solution(mesh):
    n = mesh.shape["col"]
    assert mesh.shape["row"] == n == 4
    spec = P(("eq", "row"), "col")
    return jax.shard_map(
        functools.partial(per_device, n),
        mesh=mesh,
        in_specs=(spec, spec),
        out_specs=(spec, spec),
        check_vma=False,
    )
```

```python
import functools

import jax
import jax.numpy as jnp
from jax import lax
from jax.experimental import pallas as pl
from jax.experimental.pallas import tpu as pltpu
from jax.sharding import PartitionSpec as P

CHUNKS = 8
AHEAD = 2
LATE = 1
ORDERS = (
  (
    255721738, 6686731, 38176921, 40303216, 8931872, 247220898, 152044195, 153457217,
    13051202, 26289603, 240395799, 15296849, 207122550, 146345699, 174286565, 81095224,
    64879033, 190209368, 196544347, 83469115, 181348190, 256648095, 32763879, 221911255,
    225228072, 229439017, 233649962, 111877803, 258842413, 100630318,
  ),
  (
    255721738, 6686731, 38176921, 40303216, 8931872, 247220898, 202375843, 136680024,
    59813089, 141996294, 192465804, 15295090, 156394614, 210636491, 28403292, 163017392,
    251452582, 171186334, 214861638, 175417182, 179640615, 149868502, 167244794, 219535759,
    223286377, 227349739, 231691629, 93148655, 258693950, 100630318,
  ),
  (
    245120248, 168835825, 154427592, 141732162, 248703474, 209236192, 242430532, 190213239,
    212954715, 215066333, 219277150, 228259177, 177993581, 267758287, 268435455, 268435455,
    268435455, 268435455, 268435455, 268435455, 268435455, 268435455, 268435455, 268435455,
    268435455, 268435455, 268435455, 268435455, 268435455, 268435455,
  ),
  (
    245120248, 202390257, 188244184, 141996354, 248967666, 158508232, 160903748, 212958195,
    148121309, 171159398, 224031815, 175846866, 234174317, 267758287, 268435455, 268435455,
    268435455, 268435455, 268435455, 268435455, 268435455, 268435455, 268435455, 268435455,
    268435455, 268435455, 268435455, 268435455, 268435455, 268435455,
  ),
)


def split(value):
    high = value.astype(jnp.bfloat16)
    return high, (value - high.astype(jnp.float32)).astype(jnp.bfloat16)


def product(stacked, high, low, transposed=False):
    dims = (((1,), (1 if transposed else 0,)), ((), ()))
    dot = functools.partial(lax.dot_general, dimension_numbers=dims, preferred_element_type=jnp.float32)
    step = stacked.shape[0] // 2
    both = dot(stacked, high)
    return both[:step] + (both[step:] + dot(stacked[:step], low))


def kernel(
    n, a_ref, x_ref, update_ref, square_ref,
    a_row, a_col, x_col, arrived, x_high, x_low, a_high, a_low, y_parts, lhs,
    local_sems, near_send, near_recv, far_send, far_recv, relay_send, relay_recv,
    gather_send, gather_recv, reduce_send, reduce_recv, end_send, end_recv, free_sems,
):
    r, z = lax.axis_index("row"), lax.axis_index("col")
    size = a_ref.shape[0]
    step = size // CHUNKS
    half_rows = size // 2
    last = n - 1
    pair = r // 2
    side = lax.rem(r, 2)
    far = lax.rem(r + n // 2, n)
    near = r + 1 - 2 * side
    far_near = lax.rem(near + n // 2, n)
    own_outer = jnp.where(pair == 0, 0, last)
    own_inner = jnp.where(pair == 0, 1, last - 1)
    far_outer = last - own_outer
    far_inner = last - own_inner
    at_end = (z == 0) | (z == last)
    inside = (z > 0) & (z < last)
    beside = jnp.where(z == 0, 1, last - 1)

    def rows(c):
        return pl.ds(pl.multiple_of(c * step, step), step)

    def loop(low, high, body):
        def one(i, carry):
            body(i)
            return carry

        lax.fori_loop(low, high, one, 0)

    def remote(src, dst, send, recv, **where):
        return pltpu.make_async_remote_copy(
            src_ref=src, dst_ref=dst, send_sem=send, recv_sem=recv,
            device_id=where, device_id_type=pl.DeviceIdType.MESH,
        )

    partial = x_col
    local = [
        pltpu.make_async_copy(a_ref, a_col.at[r], local_sems.at[0]),
        pltpu.make_async_copy(x_ref, x_col.at[r], local_sems.at[1]),
        pltpu.make_async_copy(x_ref, update_ref, local_sems.at[2]),
    ]
    for copy in local:
        copy.start()

    barrier = pltpu.get_barrier_semaphore()

    def greet(**where):
        pl.semaphore_signal(barrier, inc=1, device_id=where, device_id_type=pl.DeviceIdType.MESH)

    greet(row=far)
    greet(row=near)

    @pl.when(z > 0)
    def _():
        greet(col=z - 1)

    @pl.when(z < last)
    def _():
        greet(col=z + 1)

    pl.semaphore_wait(barrier, 4 - jnp.where(z == 0, 1, 0) - jnp.where(z == last, 1, 0))

    def gather_copy(right, block, c):
        slot = jnp.where(right, block, block - 1)
        landing = a_row.at[slot, rows(c)]
        sems = gather_send.at[jnp.where(right, 0, 1), jnp.abs(block - z), c], gather_recv.at[slot, c]
        to = jnp.where(right, z + 1, z - 1)
        return landing, sems, to

    def gather_own(right, c):
        landing, sems, to = gather_copy(right, z, c)
        return remote(a_col.at[r, rows(c)], landing, *sems, col=to)

    def gather_pass(right, block, c):
        landing, sems, to = gather_copy(right, block, c)
        return remote(landing, landing, *sems, col=to)

    def gather_arrival(block, c):
        slot = jnp.where(block > z, block - 1, block)
        remote(
            a_row.at[slot, rows(c)], a_row.at[slot, rows(c)],
            gather_send.at[0, 0, c], gather_recv.at[slot, c], row=near,
        ).wait_recv()

    def own_both(c):
        @pl.when(z < last)
        def _():
            gather_own(True, c).start()

        @pl.when(z > 0)
        def _():
            gather_own(False, c).start()

    def pass_gather(block, c):
        gather_arrival(block, c)
        gather_pass(block < z, block, c).start()

    def gather_end(c):
        @pl.when(at_end)
        def _():
            for hop in range(1, n):
                gather_arrival(jnp.where(z == 0, hop, last - hop), c)

    def near_copy(which):
        buffer = (x_col, a_col)[which]
        return remote(buffer.at[r], buffer.at[r], near_send.at[which], near_recv.at[which], row=near)

    def near_wait(which):
        buffer = (x_col, a_col)[which]
        remote(buffer.at[near], buffer.at[near], near_send.at[which], near_recv.at[which], row=near).wait_recv()

    def half_of(piece, mine, rows_of):
        buffer = x_col if piece < 2 else a_col
        if piece < 2:
            block = (r, near)[piece] if mine else (far, far_near)[piece]
        else:
            block = ((own_outer, own_inner) if mine else (far_outer, far_inner))[piece - 2]
        return buffer.at[block, pl.ds(pl.multiple_of(rows_of * half_rows, half_rows), half_rows)]

    def far_copy(piece):
        ref = half_of(piece, True, side)
        return remote(ref, ref, far_send.at[piece], far_recv.at[piece], row=far)

    def relay_copy(piece):
        ref = half_of(piece, False, side)
        return remote(ref, ref, relay_send.at[piece], relay_recv.at[piece], row=near)

    def relay(piece):
        ref = half_of(piece, False, side)
        remote(ref, ref, far_send.at[piece], far_recv.at[piece], row=far).wait_recv()
        relay_copy(piece).start()

    def relay_wait(piece):
        ref = half_of(piece, False, 1 - side)
        remote(ref, ref, relay_send.at[piece], relay_recv.at[piece], row=near).wait_recv()

    x_pair, a_pair = (x_high, x_low), (a_high, a_low)

    def split_rows(source, pair_refs, block, low_row, count):
        def some(i):
            at = pl.multiple_of(low_row + i * step, step)
            to = pl.ds(pl.multiple_of(block * size + at, step), step)
            pair_refs[0][to], pair_refs[1][to] = split(source[pl.ds(at, step)])

        loop(0, count // step, some)

    def split_half(block, which_half):
        split_rows(x_col.at[block], x_pair, block, which_half * half_rows, half_rows)

    def split_all(source, pair_refs, block):
        split_rows(source, pair_refs, block, 0, size)

    def multiply(c, high_ref, low_ref):
        for hop in range(n):
            block = lax.rem(z + hop, n)
            slot = jnp.where(block > z, block - 1, block)
            high, low = split(a_col[r, rows(c)] if hop == 0 else a_row[slot, rows(c)])
            to = pl.ds(pl.multiple_of(block * size, size), size)
            lhs[:step, to] = high
            lhs[step:, to] = low
        return product(lhs[...], high_ref[...], low_ref[...])

    def y_rows(c):
        return pl.ds(pl.multiple_of(c * 2 * step, 2 * step), 2 * step)

    def compute_y(c):
        value = multiply(c, x_high, x_low)

        @pl.when(at_end & (c >= CHUNKS - LATE))
        def _():
            partial[beside, rows(c)] = value

        high, low = split(value)
        base = pl.multiple_of(c * 2 * step, 2 * step)
        y_parts[pl.ds(base, step)] = high
        y_parts[pl.ds(pl.multiple_of(base + step, step), step)] = low

    def compute_square(c):
        square_ref[rows(c)] = multiply(c, a_high, a_low)

    def reduce_copy(right, d, c):
        target = jnp.where(right, z + 1, z - 1)
        slot = jnp.where(right & (d == target), n, d)
        return remote(
            partial.at[d, rows(c)], arrived.at[slot, rows(c)],
            reduce_send.at[d, c], reduce_recv.at[slot, c], col=target,
        )

    def reduce_wait(slot, c):
        remote(
            arrived.at[slot, rows(c)], arrived.at[slot, rows(c)],
            reduce_send.at[0, c], reduce_recv.at[slot, c], row=near,
        ).wait_recv()

    def compute_partial(c, d):
        block = pl.ds(pl.multiple_of(d * size, size), size)
        partial[d, rows(c)] = product(y_parts[y_rows(c)], a_high[block], a_low[block], transposed=True)

        @pl.when(((z == 0) & (d > 0)) | ((z == last) & (d < last)))
        def _():
            reduce_copy(z == 0, d, c).start()

    def pass_piece(d, c):
        reduce_wait(d, c)
        partial[d, rows(c)] = partial[d, rows(c)] + arrived[d, rows(c)]
        reduce_copy(d > z, d, c).start()

    def landed(piece):
        relay_wait(piece)
        if piece < 2:
            split_half((far, far_near)[piece], side)
            split_half((far_near, far)[piece], 1 - side)
        else:
            block = (far_outer, far_inner)[piece - 2]
            split_all(a_col.at[block], a_pair, block)
        if piece == 1:
            near_copy(0).wait_send()
            for sent_piece in range(2):
                far_copy(sent_piece).wait_send()
                relay_copy(sent_piece).wait_send()
        if piece == 3:
            for sent_piece in range(2, 4):
                far_copy(sent_piece).wait_send()
                relay_copy(sent_piece).wait_send()

            @pl.when(inside)
            def _():
                for at, row in ((0, near), (1, far)):
                    pl.semaphore_signal(
                        free_sems.at[at], inc=1, device_id={"row": row}, device_id_type=pl.DeviceIdType.MESH
                    )

    mirrored = z >= n // 2
    end_slot = jnp.where(mirrored, n - 2, 0)

    def end_copy(which):
        source, block, row = (
            (a_row.at[end_slot], r, far), (a_row.at[end_slot], r, near), (a_col.at[far], far, near)
        )[which]
        return remote(source, a_col.at[block], end_send.at[which], end_recv.at[which], row=row)

    def end_wait(which):
        block = (far, near, far_near)[which]
        remote(a_col.at[block], a_col.at[block], end_send.at[which], end_recv.at[which], row=near).wait_recv()

    def end_start():
        pl.semaphore_wait(free_sems.at[0], 1)
        pl.semaphore_wait(free_sems.at[1], 1)
        end_copy(0).start()
        end_copy(1).start()

    def end_middle():
        end_wait(0)
        end_copy(2).start()
        split_all(a_row.at[end_slot], x_pair, r)
        end_wait(1)
        split_all(a_col.at[near], x_pair, near)
        split_all(a_col.at[far], x_pair, far)

    def end_last():
        end_wait(2)
        split_all(a_col.at[far_near], x_pair, far_near)

    def end_partials(c):
        slot = jnp.where(mirrored, z, n)
        reduce_wait(slot, c)
        high, low = split(arrived[slot, rows(c)])
        lhs[:step, :size] = high
        lhs[step:, :size] = low

        def one(i):
            d = jnp.where(mirrored, i, last - i)
            block = pl.ds(pl.multiple_of(d * size, size), size)
            partial[d, rows(c)] = partial[d, rows(c)] + product(
                lhs[:, :size], x_high[block], x_low[block], transposed=True
            )

            @pl.when(i < n // 2)
            def _():
                reduce_copy(d > z, d, c).start()

        loop(0, n - 1, one)

    def facing(index):
        return jnp.where(mirrored, last - index, index)

    def other(index):
        return facing(jnp.where(index >= 1, index + 1, index))

    def act(code):
        def when(low, count, body):
            @pl.when((code >= low) & (code < low + count))
            def _():
                body((code - low) // CHUNKS, lax.rem(code - low, CHUNKS))

        def once(value, body):
            @pl.when(code == value)
            def _():
                body()

        when(0, 2 * CHUNKS, lambda i, c: gather_own((i == 0) != mirrored, c).start())
        when(16, 3 * CHUNKS, lambda i, c: pass_gather(other(i), c))
        when(40, 3 * CHUNKS, lambda i, c: pass_piece(other(i), c))

        def begin(i, c):
            gather_end(c)
            compute_y(c)

            @pl.when(at_end & (c >= CHUNKS - LATE))
            def _():
                reduce_copy(z == 0, beside, c).start()

        when(64, CHUNKS, begin)
        when(72, 4 * CHUNKS, lambda i, c: compute_partial(c, facing(i)))
        when(104, CHUNKS, lambda i, c: compute_square(c))
        for piece in range(4):
            once(112 + piece, functools.partial(relay, piece))
            once(116 + piece, functools.partial(landed, piece))
        once(120, lambda: split_both(x_col, x_pair))
        once(121, lambda: split_both(a_col, a_pair))
        once(122, end_start)
        once(123, end_middle)
        once(126, end_last)
        once(125, lambda: end_partials(CHUNKS - 1))

    def split_both(source, pair_refs):
        def one(i):
            block = jnp.where(i == 0, r, near)
            split_all(source.at[block], pair_refs, block)

        loop(0, 2, one)

    local[1].wait()
    far_copy(0).start()
    near_copy(0).start()
    local[0].wait()

    @pl.when(at_end)
    def _():
        loop(0, CHUNKS, own_both)

    @pl.when(inside)
    def _():
        loop(0, AHEAD, own_both)

    near_copy(1).start()
    near_wait(0)
    far_copy(1).start()
    near_wait(1)
    far_copy(2).start()
    far_copy(3).start()

    second = (pair == 0) == mirrored
    choice = jnp.where(at_end, 2, 0) + jnp.where(second, 1, 0)

    def four(i):
        word = 0
        for at in range(len(ORDERS[0])):
            value = ORDERS[3][at]
            for v in range(3):
                value = jnp.where(choice == v, ORDERS[v][at], value)
            word = jnp.where(i == at, value, word)

        def one(j, left):
            act(lax.rem(left, 128))
            return left // 128

        lax.fori_loop(0, 4, one, word)

    loop(0, len(ORDERS[0]), four)

    def finish(c):
        update_ref[rows(c)] = update_ref[rows(c)] + partial[z, rows(c)]

        early = c < CHUNKS - LATE

        @pl.when((z < last) & (early | (z != last - 1)))
        def _():
            reduce_wait(z, c)
            update_ref[rows(c)] = update_ref[rows(c)] + arrived[z, rows(c)]

        @pl.when((z > 0) & (early | (z != 1)))
        def _():
            reduce_wait(n, c)
            update_ref[rows(c)] = update_ref[rows(c)] + arrived[n, rows(c)]

    local[2].wait()
    loop(0, CHUNKS, finish)

    near_copy(1).wait_send()

    @pl.when(inside)
    def _():
        for which in range(3):
            end_copy(which).wait_send()

    def sent(c):
        for hop in range(n - 1):
            @pl.when((z < last) & (z - hop >= 0))
            def _():
                gather_pass(True, z - hop, c).wait_send()

            @pl.when((z > 0) & (z + hop <= last))
            def _():
                gather_pass(False, z + hop, c).wait_send()

        for d in range(n):
            @pl.when((z != d) & (inside | (c < CHUNKS - LATE) | (d == beside)))
            def _():
                reduce_copy(z < d, d, c).wait_send()

    loop(0, CHUNKS, sent)


def per_device(n, transition, covariance):
    size = transition.shape[0]
    f32, bf16 = jnp.float32, jnp.bfloat16
    shape = jax.ShapeDtypeStruct(transition.shape, f32)
    return pl.pallas_call(
        functools.partial(kernel, n),
        out_shape=(pltpu.VMEM(transition.shape, f32),) * 2,
        in_specs=[pl.BlockSpec(memory_space=pl.ANY)] * 2,
        out_specs=(pl.BlockSpec(memory_space=pltpu.VMEM),) * 2,
        scratch_shapes=[
            pltpu.VMEM((n - 1, size, size), f32),
            pltpu.VMEM((n, size, size), f32),
            pltpu.VMEM((n, size, size), f32),
            pltpu.VMEM((n + 1, size, size), f32),
            pltpu.VMEM((n * size, size), bf16),
            pltpu.VMEM((n * size, size), bf16),
            pltpu.VMEM((n * size, size), bf16),
            pltpu.VMEM((n * size, size), bf16),
            pltpu.VMEM((2 * size, size), bf16),
            pltpu.VMEM((2 * size // CHUNKS, n * size), bf16),
            pltpu.SemaphoreType.DMA((3,)),
            pltpu.SemaphoreType.DMA((2,)),
            pltpu.SemaphoreType.DMA((2,)),
            pltpu.SemaphoreType.DMA((4,)),
            pltpu.SemaphoreType.DMA((4,)),
            pltpu.SemaphoreType.DMA((4,)),
            pltpu.SemaphoreType.DMA((4,)),
            pltpu.SemaphoreType.DMA((2, n - 1, CHUNKS)),
            pltpu.SemaphoreType.DMA((n - 1, CHUNKS)),
            pltpu.SemaphoreType.DMA((n, CHUNKS)),
            pltpu.SemaphoreType.DMA((n + 1, CHUNKS)),
            pltpu.SemaphoreType.DMA((3,)),
            pltpu.SemaphoreType.DMA((3,)),
            pltpu.SemaphoreType.REGULAR((2,)),
        ],
        compiler_params=pltpu.CompilerParams(
            collective_id=0, has_side_effects=True, vmem_limit_bytes=67043328 - 2 * 4 * transition.size
        ),
    )(transition, covariance)


def solution(mesh):
    n = mesh.shape["col"]
    assert mesh.shape["row"] == n == 4
    spec = P(("eq", "row"), "col")
    return jax.shard_map(
        functools.partial(per_device, n),
        mesh=mesh,
        in_specs=(spec, spec),
        out_specs=(spec, spec),
        check_vma=False,
    )
```

```python
import functools

import jax
import jax.numpy as jnp
from jax import lax
from jax.experimental import pallas as pl
from jax.experimental.pallas import tpu as pltpu
from jax.sharding import PartitionSpec as P

CHUNKS = 8
AHEAD = 2
LATE = 1
ORDERS = (
  (
    33733880, 36061464, 245106970, 6834592, 8964642, 44497649, 24142912, 156279941,
    158386980, 13052112, 173226308, 203262860, 79229281, 177533447, 119104157, 119761613,
    256490483, 190209368, 196546395, 197370683, 181640806, 149411879, 167368927, 106572687,
    108696681, 110826731, 129733997, 264952571, 95393391, 99456893,
  ),
  (
    33733880, 36061464, 245106970, 6834592, 8964642, 44497649, 24522816, 204890245,
    205886018, 13050330, 144485859, 152931212, 78832969, 160903687, 212950045, 100886237,
    120175603, 173303930, 147754835, 103001958, 181758542, 105373095, 167244743, 219536911,
    223138921, 227172075, 231560557, 265098747, 93020015, 99456893,
  ),
  (
    245120248, 137378545, 173302096, 141731016, 248703474, 209236192, 242430532, 190213239,
    162623067, 196699974, 221914086, 228046314, 234596973, 267757525, 268435455, 268435455,
    268435455, 268435455, 268435455, 268435455, 268435455, 268435455, 268435455, 268435455,
    268435455, 268435455, 268435455, 268435455, 268435455, 268435455,
  ),
  (
    245120248, 185613041, 188244192, 141996354, 248967666, 158508232, 161033796, 146029555,
    213165777, 175353542, 221914086, 228257642, 180074196, 267757551, 268435455, 268435455,
    268435455, 268435455, 268435455, 268435455, 268435455, 268435455, 268435455, 268435455,
    268435455, 268435455, 268435455, 268435455, 268435455, 268435455,
  ),
)


def split(value):
    high = value.astype(jnp.bfloat16)
    return high, (value - high.astype(jnp.float32)).astype(jnp.bfloat16)


def product(stacked, high, low, transposed=False):
    dims = (((1,), (1 if transposed else 0,)), ((), ()))
    dot = functools.partial(lax.dot_general, dimension_numbers=dims, preferred_element_type=jnp.float32)
    step = stacked.shape[0] // 2
    both = dot(stacked, high)
    return both[:step] + (both[step:] + dot(stacked[:step], low))


def kernel(
    n, a_ref, x_ref, update_ref, square_ref,
    a_row, a_col, x_col, arrived, x_high, x_low, a_high, a_low, y_parts, lhs,
    local_sems, near_send, near_recv, far_send, far_recv, relay_send, relay_recv,
    gather_send, gather_recv, reduce_send, reduce_recv, end_send, end_recv, free_sems,
):
    r, z = lax.axis_index("row"), lax.axis_index("col")
    size = a_ref.shape[0]
    step = size // CHUNKS
    half_rows = size // 2
    last = n - 1
    pair = r // 2
    side = lax.rem(r, 2)
    far = lax.rem(r + n // 2, n)
    near = r + 1 - 2 * side
    far_near = lax.rem(near + n // 2, n)
    own_outer = jnp.where(pair == 0, 0, last)
    own_inner = jnp.where(pair == 0, 1, last - 1)
    far_outer = last - own_outer
    far_inner = last - own_inner
    at_end = (z == 0) | (z == last)
    inside = (z > 0) & (z < last)
    beside = jnp.where(z == 0, 1, last - 1)

    def rows(c):
        return pl.ds(pl.multiple_of(c * step, step), step)

    def loop(low, high, body):
        def one(i, carry):
            body(i)
            return carry

        lax.fori_loop(low, high, one, 0)

    def remote(src, dst, send, recv, **where):
        return pltpu.make_async_remote_copy(
            src_ref=src, dst_ref=dst, send_sem=send, recv_sem=recv,
            device_id=where, device_id_type=pl.DeviceIdType.MESH,
        )

    partial = x_col
    local = [
        pltpu.make_async_copy(a_ref, a_col.at[r], local_sems.at[0]),
        pltpu.make_async_copy(x_ref, x_col.at[r], local_sems.at[1]),
        pltpu.make_async_copy(x_ref, update_ref, local_sems.at[2]),
    ]
    for copy in local:
        copy.start()

    barrier = pltpu.get_barrier_semaphore()

    def greet(**where):
        pl.semaphore_signal(barrier, inc=1, device_id=where, device_id_type=pl.DeviceIdType.MESH)

    greet(row=far)
    greet(row=near)

    @pl.when(z > 0)
    def _():
        greet(col=z - 1)

    @pl.when(z < last)
    def _():
        greet(col=z + 1)

    pl.semaphore_wait(barrier, 4 - jnp.where(z == 0, 1, 0) - jnp.where(z == last, 1, 0))

    def gather_copy(right, block, c):
        slot = jnp.where(right, block, block - 1)
        landing = a_row.at[slot, rows(c)]
        sems = gather_send.at[jnp.where(right, 0, 1), jnp.abs(block - z), c], gather_recv.at[slot, c]
        to = jnp.where(right, z + 1, z - 1)
        return landing, sems, to

    def gather_own(right, c):
        landing, sems, to = gather_copy(right, z, c)
        return remote(a_col.at[r, rows(c)], landing, *sems, col=to)

    def gather_pass(right, block, c):
        landing, sems, to = gather_copy(right, block, c)
        return remote(landing, landing, *sems, col=to)

    def gather_arrival(block, c):
        slot = jnp.where(block > z, block - 1, block)
        remote(
            a_row.at[slot, rows(c)], a_row.at[slot, rows(c)],
            gather_send.at[0, 0, c], gather_recv.at[slot, c], row=near,
        ).wait_recv()

    def own_both(c):
        @pl.when(z < last)
        def _():
            gather_own(True, c).start()

        @pl.when(z > 0)
        def _():
            gather_own(False, c).start()

    def pass_gather(block, c):
        gather_arrival(block, c)
        gather_pass(block < z, block, c).start()

    def gather_end(c):
        @pl.when(at_end)
        def _():
            for hop in range(1, n):
                gather_arrival(jnp.where(z == 0, hop, last - hop), c)

    def near_copy(which):
        buffer = (x_col, a_col)[which]
        return remote(buffer.at[r], buffer.at[r], near_send.at[which], near_recv.at[which], row=near)

    def near_wait(which):
        buffer = (x_col, a_col)[which]
        remote(buffer.at[near], buffer.at[near], near_send.at[which], near_recv.at[which], row=near).wait_recv()

    def half_of(piece, mine, rows_of):
        buffer = x_col if piece < 2 else a_col
        if piece < 2:
            block = (r, near)[piece] if mine else (far, far_near)[piece]
        else:
            block = ((own_outer, own_inner) if mine else (far_outer, far_inner))[piece - 2]
        return buffer.at[block, pl.ds(pl.multiple_of(rows_of * half_rows, half_rows), half_rows)]

    def far_copy(piece):
        ref = half_of(piece, True, side)
        return remote(ref, ref, far_send.at[piece], far_recv.at[piece], row=far)

    def relay_copy(piece):
        ref = half_of(piece, False, side)
        return remote(ref, ref, relay_send.at[piece], relay_recv.at[piece], row=near)

    def relay(piece):
        ref = half_of(piece, False, side)
        remote(ref, ref, far_send.at[piece], far_recv.at[piece], row=far).wait_recv()
        relay_copy(piece).start()

    def relay_wait(piece):
        ref = half_of(piece, False, 1 - side)
        remote(ref, ref, relay_send.at[piece], relay_recv.at[piece], row=near).wait_recv()

    x_pair, a_pair = (x_high, x_low), (a_high, a_low)

    def split_rows(source, pair_refs, block, low_row, count):
        def some(i):
            at = pl.multiple_of(low_row + i * step, step)
            to = pl.ds(pl.multiple_of(block * size + at, step), step)
            pair_refs[0][to], pair_refs[1][to] = split(source[pl.ds(at, step)])

        loop(0, count // step, some)

    def split_half(block, which_half):
        split_rows(x_col.at[block], x_pair, block, which_half * half_rows, half_rows)

    def split_all(source, pair_refs, block):
        split_rows(source, pair_refs, block, 0, size)

    def multiply(c, high_ref, low_ref):
        for hop in range(n):
            block = lax.rem(z + hop, n)
            slot = jnp.where(block > z, block - 1, block)
            high, low = split(a_col[r, rows(c)] if hop == 0 else a_row[slot, rows(c)])
            to = pl.ds(pl.multiple_of(block * size, size), size)
            lhs[:step, to] = high
            lhs[step:, to] = low
        return product(lhs[...], high_ref[...], low_ref[...])

    def y_rows(c):
        return pl.ds(pl.multiple_of(c * 2 * step, 2 * step), 2 * step)

    def compute_y(c):
        value = multiply(c, x_high, x_low)

        @pl.when(at_end & (c >= CHUNKS - LATE))
        def _():
            partial[beside, rows(c)] = value

        high, low = split(value)
        base = pl.multiple_of(c * 2 * step, 2 * step)
        y_parts[pl.ds(base, step)] = high
        y_parts[pl.ds(pl.multiple_of(base + step, step), step)] = low

    def compute_square(c):
        square_ref[rows(c)] = multiply(c, a_high, a_low)

    def reduce_copy(right, d, c):
        target = jnp.where(right, z + 1, z - 1)
        slot = jnp.where(right & (d == target), n, d)
        return remote(
            partial.at[d, rows(c)], arrived.at[slot, rows(c)],
            reduce_send.at[d, c], reduce_recv.at[slot, c], col=target,
        )

    def reduce_wait(slot, c):
        remote(
            arrived.at[slot, rows(c)], arrived.at[slot, rows(c)],
            reduce_send.at[0, c], reduce_recv.at[slot, c], row=near,
        ).wait_recv()

    def compute_partial(c, d):
        block = pl.ds(pl.multiple_of(d * size, size), size)
        partial[d, rows(c)] = product(y_parts[y_rows(c)], a_high[block], a_low[block], transposed=True)

        @pl.when(((z == 0) & (d > 0)) | ((z == last) & (d < last)))
        def _():
            reduce_copy(z == 0, d, c).start()

    def pass_piece(d, c):
        reduce_wait(d, c)
        partial[d, rows(c)] = partial[d, rows(c)] + arrived[d, rows(c)]
        reduce_copy(d > z, d, c).start()

    def landed(piece):
        relay_wait(piece)
        if piece < 2:
            split_half((far, far_near)[piece], side)
            split_half((far_near, far)[piece], 1 - side)
        else:
            block = (far_outer, far_inner)[piece - 2]
            split_all(a_col.at[block], a_pair, block)
        if piece == 1:
            near_copy(0).wait_send()
            for sent_piece in range(2):
                far_copy(sent_piece).wait_send()
                relay_copy(sent_piece).wait_send()
        if piece == 3:
            for sent_piece in range(2, 4):
                far_copy(sent_piece).wait_send()
                relay_copy(sent_piece).wait_send()

            @pl.when(inside)
            def _():
                for at, row in ((0, near), (1, far)):
                    pl.semaphore_signal(
                        free_sems.at[at], inc=1, device_id={"row": row}, device_id_type=pl.DeviceIdType.MESH
                    )

    mirrored = z >= n // 2
    end_slot = jnp.where(mirrored, n - 2, 0)

    def end_copy(which):
        source, block, row = (
            (a_row.at[end_slot], r, far), (a_row.at[end_slot], r, near), (a_col.at[far], far, near)
        )[which]
        return remote(source, a_col.at[block], end_send.at[which], end_recv.at[which], row=row)

    def end_wait(which):
        block = (far, near, far_near)[which]
        remote(a_col.at[block], a_col.at[block], end_send.at[which], end_recv.at[which], row=near).wait_recv()

    def end_start():
        pl.semaphore_wait(free_sems.at[0], 1)
        pl.semaphore_wait(free_sems.at[1], 1)
        end_copy(0).start()
        end_copy(1).start()

    def end_middle():
        end_wait(0)
        end_copy(2).start()
        split_all(a_row.at[end_slot], x_pair, r)
        end_wait(1)
        split_all(a_col.at[near], x_pair, near)
        split_all(a_col.at[far], x_pair, far)

    def end_last():
        end_wait(2)
        split_all(a_col.at[far_near], x_pair, far_near)

    def end_partials(c):
        slot = jnp.where(mirrored, z, n)
        reduce_wait(slot, c)
        high, low = split(arrived[slot, rows(c)])
        lhs[:step, :size] = high
        lhs[step:, :size] = low

        def one(i):
            d = jnp.where(mirrored, i, last - i)
            block = pl.ds(pl.multiple_of(d * size, size), size)
            partial[d, rows(c)] = partial[d, rows(c)] + product(
                lhs[:, :size], x_high[block], x_low[block], transposed=True
            )

            @pl.when(i < n // 2)
            def _():
                reduce_copy(d > z, d, c).start()

        loop(0, n - 1, one)

    def facing(index):
        return jnp.where(mirrored, last - index, index)

    def other(index):
        return facing(jnp.where(index >= 1, index + 1, index))

    def act(code):
        def when(low, count, body):
            @pl.when((code >= low) & (code < low + count))
            def _():
                body((code - low) // CHUNKS, lax.rem(code - low, CHUNKS))

        def once(value, body):
            @pl.when(code == value)
            def _():
                body()

        when(0, 2 * CHUNKS, lambda i, c: gather_own((i == 0) != mirrored, c).start())
        when(16, 3 * CHUNKS, lambda i, c: pass_gather(other(i), c))
        when(40, 3 * CHUNKS, lambda i, c: pass_piece(other(i), c))

        def begin(i, c):
            gather_end(c)
            compute_y(c)

            @pl.when(at_end & (c >= CHUNKS - LATE))
            def _():
                reduce_copy(z == 0, beside, c).start()

        when(64, CHUNKS, begin)
        when(72, 4 * CHUNKS, lambda i, c: compute_partial(c, facing(i)))
        when(104, CHUNKS, lambda i, c: compute_square(c))
        for piece in range(4):
            once(112 + piece, functools.partial(relay, piece))
            once(116 + piece, functools.partial(landed, piece))
        once(120, lambda: split_both(x_col, x_pair))
        once(121, lambda: split_both(a_col, a_pair))
        once(122, end_start)
        once(123, end_middle)
        once(126, end_last)
        once(125, lambda: end_partials(CHUNKS - 1))

    def split_both(source, pair_refs):
        def one(i):
            block = jnp.where(i == 0, r, near)
            split_all(source.at[block], pair_refs, block)

        loop(0, 2, one)

    local[1].wait()
    far_copy(0).start()
    near_copy(0).start()
    local[0].wait()

    @pl.when(at_end)
    def _():
        loop(0, CHUNKS, own_both)

    @pl.when(inside)
    def _():
        loop(0, AHEAD, own_both)

    near_copy(1).start()
    near_wait(0)
    far_copy(1).start()
    near_wait(1)
    far_copy(2).start()
    far_copy(3).start()

    second = (pair == 0) == mirrored
    choice = jnp.where(at_end, 2, 0) + jnp.where(second, 1, 0)

    def four(i):
        word = 0
        for at in range(len(ORDERS[0])):
            value = ORDERS[3][at]
            for v in range(3):
                value = jnp.where(choice == v, ORDERS[v][at], value)
            word = jnp.where(i == at, value, word)

        def one(j, left):
            act(lax.rem(left, 128))
            return left // 128

        lax.fori_loop(0, 4, one, word)

    loop(0, len(ORDERS[0]), four)

    def finish(c):
        update_ref[rows(c)] = update_ref[rows(c)] + partial[z, rows(c)]

        early = c < CHUNKS - LATE

        @pl.when((z < last) & (early | (z != last - 1)))
        def _():
            reduce_wait(z, c)
            update_ref[rows(c)] = update_ref[rows(c)] + arrived[z, rows(c)]

        @pl.when((z > 0) & (early | (z != 1)))
        def _():
            reduce_wait(n, c)
            update_ref[rows(c)] = update_ref[rows(c)] + arrived[n, rows(c)]

    local[2].wait()
    loop(0, CHUNKS - 1, finish)

    near_copy(1).wait_send()

    @pl.when(inside)
    def _():
        for which in range(3):
            end_copy(which).wait_send()

    def sent(c):
        for hop in range(n - 1):
            @pl.when((z < last) & (z - hop >= 0))
            def _():
                gather_pass(True, z - hop, c).wait_send()

            @pl.when((z > 0) & (z + hop <= last))
            def _():
                gather_pass(False, z + hop, c).wait_send()

        for d in range(n):
            @pl.when((z != d) & (inside | (c < CHUNKS - LATE) | (d == beside)))
            def _():
                reduce_copy(z < d, d, c).wait_send()

    loop(0, CHUNKS, sent)
    finish(CHUNKS - 1)


def per_device(n, transition, covariance):
    size = transition.shape[0]
    f32, bf16 = jnp.float32, jnp.bfloat16
    return pl.pallas_call(
        functools.partial(kernel, n),
        out_shape=(pltpu.VMEM(transition.shape, f32),) * 2,
        in_specs=[pl.BlockSpec(memory_space=pl.ANY)] * 2,
        out_specs=(pl.BlockSpec(memory_space=pltpu.VMEM),) * 2,
        scratch_shapes=[
            pltpu.VMEM((n - 1, size, size), f32),
            pltpu.VMEM((n, size, size), f32),
            pltpu.VMEM((n, size, size), f32),
            pltpu.VMEM((n + 1, size, size), f32),
            pltpu.VMEM((n * size, size), bf16),
            pltpu.VMEM((n * size, size), bf16),
            pltpu.VMEM((n * size, size), bf16),
            pltpu.VMEM((n * size, size), bf16),
            pltpu.VMEM((2 * size, size), bf16),
            pltpu.VMEM((2 * size // CHUNKS, n * size), bf16),
            pltpu.SemaphoreType.DMA((3,)),
            pltpu.SemaphoreType.DMA((2,)),
            pltpu.SemaphoreType.DMA((2,)),
            pltpu.SemaphoreType.DMA((4,)),
            pltpu.SemaphoreType.DMA((4,)),
            pltpu.SemaphoreType.DMA((4,)),
            pltpu.SemaphoreType.DMA((4,)),
            pltpu.SemaphoreType.DMA((2, n - 1, CHUNKS)),
            pltpu.SemaphoreType.DMA((n - 1, CHUNKS)),
            pltpu.SemaphoreType.DMA((n, CHUNKS)),
            pltpu.SemaphoreType.DMA((n + 1, CHUNKS)),
            pltpu.SemaphoreType.DMA((3,)),
            pltpu.SemaphoreType.DMA((3,)),
            pltpu.SemaphoreType.REGULAR((2,)),
        ],
        compiler_params=pltpu.CompilerParams(
            collective_id=0, has_side_effects=True, vmem_limit_bytes=67043328 - 2 * 4 * transition.size
        ),
    )(transition, covariance)


def solution(mesh):
    n = mesh.shape["col"]
    assert mesh.shape["row"] == n == 4
    spec = P(("eq", "row"), "col")
    return jax.shard_map(
        functools.partial(per_device, n),
        mesh=mesh,
        in_specs=(spec, spec),
        out_specs=(spec, spec),
        check_vma=False,
    )
```

```python
import functools

import jax
import jax.numpy as jnp
from jax import lax
from jax.experimental import pallas as pl
from jax.experimental.pallas import tpu as pltpu
from jax.sharding import PartitionSpec as P

CHUNKS = 8
AHEAD = 2
LATE = 1
ORDERS = (
  (
    33733880, 36061464, 245106970, 6834592, 8964642, 44497649, 24142912, 156279941,
    158386980, 13052112, 173226308, 203262860, 79229281, 177533447, 119104157, 119761613,
    256490483, 190209368, 196546395, 197370683, 181640806, 149411879, 167368927, 106572687,
    108696681, 110826731, 129733997, 264952571, 95393391, 99456893,
  ),
  (
    33733880, 36061464, 245106970, 6834592, 8964642, 44497649, 24522816, 204890245,
    205886018, 13050330, 144485859, 152931212, 78832969, 160903687, 212950045, 100886237,
    120175603, 173303930, 147754835, 103001958, 181758542, 105373095, 167244743, 219536911,
    223138921, 227172075, 231560557, 265098747, 93020015, 99456893,
  ),
  (
    245120248, 137378545, 173302096, 141731016, 248703474, 209236192, 242430532, 190213239,
    162623067, 196699974, 221914086, 228046314, 234596973, 267757525, 268435455, 268435455,
    268435455, 268435455, 268435455, 268435455, 268435455, 268435455, 268435455, 268435455,
    268435455, 268435455, 268435455, 268435455, 268435455, 268435455,
  ),
  (
    245120248, 185613041, 188244192, 141996354, 248967666, 158508232, 161033796, 146029555,
    213165777, 175353542, 221914086, 228257642, 180074196, 267757551, 268435455, 268435455,
    268435455, 268435455, 268435455, 268435455, 268435455, 268435455, 268435455, 268435455,
    268435455, 268435455, 268435455, 268435455, 268435455, 268435455,
  ),
)


def split(value):
    high = value.astype(jnp.bfloat16)
    return high, (value - high.astype(jnp.float32)).astype(jnp.bfloat16)


def product(stacked, high, low, transposed=False):
    dims = (((1,), (1 if transposed else 0,)), ((), ()))
    dot = functools.partial(lax.dot_general, dimension_numbers=dims, preferred_element_type=jnp.float32)
    step = stacked.shape[0] // 2
    both = dot(stacked, high)
    return both[:step] + (both[step:] + dot(stacked[:step], low))


def kernel(
    n, a_ref, x_ref, update_ref, square_ref,
    a_row, a_col, x_col, arrived, x_high, x_low, a_high, a_low, y_parts, lhs,
    local_sems, near_send, near_recv, far_send, far_recv, relay_send, relay_recv,
    gather_send, gather_recv, reduce_send, reduce_recv, end_send, end_recv, free_sems,
):
    r, z = lax.axis_index("row"), lax.axis_index("col")
    size = a_ref.shape[0]
    step = size // CHUNKS
    half_rows = size // 2
    last = n - 1
    pair = r // 2
    side = lax.rem(r, 2)
    far = lax.rem(r + n // 2, n)
    near = r + 1 - 2 * side
    far_near = lax.rem(near + n // 2, n)
    own_outer = jnp.where(pair == 0, 0, last)
    own_inner = jnp.where(pair == 0, 1, last - 1)
    far_outer = last - own_outer
    far_inner = last - own_inner
    at_end = (z == 0) | (z == last)
    inside = (z > 0) & (z < last)
    beside = jnp.where(z == 0, 1, last - 1)

    def rows(c):
        return pl.ds(pl.multiple_of(c * step, step), step)

    def loop(low, high, body):
        def one(i, carry):
            body(i)
            return carry

        lax.fori_loop(low, high, one, 0)

    def remote(src, dst, send, recv, **where):
        return pltpu.make_async_remote_copy(
            src_ref=src, dst_ref=dst, send_sem=send, recv_sem=recv,
            device_id=where, device_id_type=pl.DeviceIdType.MESH,
        )

    partial = x_col
    local = [
        pltpu.make_async_copy(a_ref, a_col.at[r], local_sems.at[0]),
        pltpu.make_async_copy(x_ref, x_col.at[r], local_sems.at[1]),
        pltpu.make_async_copy(x_ref, update_ref, local_sems.at[2]),
    ]
    for copy in local[:2]:
        copy.start()

    barrier = pltpu.get_barrier_semaphore()

    def greet(**where):
        pl.semaphore_signal(barrier, inc=1, device_id=where, device_id_type=pl.DeviceIdType.MESH)

    greet(row=far)
    greet(row=near)

    @pl.when(z > 0)
    def _():
        greet(col=z - 1)

    @pl.when(z < last)
    def _():
        greet(col=z + 1)

    pl.semaphore_wait(barrier, 4 - jnp.where(z == 0, 1, 0) - jnp.where(z == last, 1, 0))

    def gather_copy(right, block, c):
        slot = jnp.where(right, block, block - 1)
        landing = a_row.at[slot, rows(c)]
        sems = gather_send.at[jnp.where(right, 0, 1), jnp.abs(block - z), c], gather_recv.at[slot, c]
        to = jnp.where(right, z + 1, z - 1)
        return landing, sems, to

    def gather_own(right, c):
        landing, sems, to = gather_copy(right, z, c)
        return remote(a_ref.at[rows(c)], landing, *sems, col=to)

    def gather_pass(right, block, c):
        landing, sems, to = gather_copy(right, block, c)
        return remote(landing, landing, *sems, col=to)

    def gather_arrival(block, c):
        slot = jnp.where(block > z, block - 1, block)
        remote(
            a_row.at[slot, rows(c)], a_row.at[slot, rows(c)],
            gather_send.at[0, 0, c], gather_recv.at[slot, c], row=near,
        ).wait_recv()

    def own_both(c):
        @pl.when(z < last)
        def _():
            gather_own(True, c).start()

        @pl.when(z > 0)
        def _():
            gather_own(False, c).start()

    def pass_gather(block, c):
        gather_arrival(block, c)
        gather_pass(block < z, block, c).start()

    def gather_end(c):
        @pl.when(at_end)
        def _():
            for hop in range(1, n):
                gather_arrival(jnp.where(z == 0, hop, last - hop), c)

    def near_copy(which):
        buffer = (x_col, a_col)[which]
        return remote(buffer.at[r], buffer.at[r], near_send.at[which], near_recv.at[which], row=near)

    def near_wait(which):
        buffer = (x_col, a_col)[which]
        remote(buffer.at[near], buffer.at[near], near_send.at[which], near_recv.at[which], row=near).wait_recv()

    def half_of(piece, mine, rows_of):
        buffer = x_col if piece < 2 else a_col
        if piece < 2:
            block = (r, near)[piece] if mine else (far, far_near)[piece]
        else:
            block = ((own_outer, own_inner) if mine else (far_outer, far_inner))[piece - 2]
        return buffer.at[block, pl.ds(pl.multiple_of(rows_of * half_rows, half_rows), half_rows)]

    def far_copy(piece):
        ref = half_of(piece, True, side)
        return remote(ref, ref, far_send.at[piece], far_recv.at[piece], row=far)

    def relay_copy(piece):
        ref = half_of(piece, False, side)
        return remote(ref, ref, relay_send.at[piece], relay_recv.at[piece], row=near)

    def relay(piece):
        ref = half_of(piece, False, side)
        remote(ref, ref, far_send.at[piece], far_recv.at[piece], row=far).wait_recv()
        relay_copy(piece).start()

    def relay_wait(piece):
        ref = half_of(piece, False, 1 - side)
        remote(ref, ref, relay_send.at[piece], relay_recv.at[piece], row=near).wait_recv()

    x_pair, a_pair = (x_high, x_low), (a_high, a_low)

    def split_rows(source, pair_refs, block, low_row, count):
        def some(i):
            at = pl.multiple_of(low_row + i * step, step)
            to = pl.ds(pl.multiple_of(block * size + at, step), step)
            pair_refs[0][to], pair_refs[1][to] = split(source[pl.ds(at, step)])

        loop(0, count // step, some)

    def split_half(block, which_half):
        split_rows(x_col.at[block], x_pair, block, which_half * half_rows, half_rows)

    def split_all(source, pair_refs, block):
        split_rows(source, pair_refs, block, 0, size)

    def multiply(c, high_ref, low_ref):
        for hop in range(n):
            block = lax.rem(z + hop, n)
            slot = jnp.where(block > z, block - 1, block)
            high, low = split(a_col[r, rows(c)] if hop == 0 else a_row[slot, rows(c)])
            to = pl.ds(pl.multiple_of(block * size, size), size)
            lhs[:step, to] = high
            lhs[step:, to] = low
        return product(lhs[...], high_ref[...], low_ref[...])

    def y_rows(c):
        return pl.ds(pl.multiple_of(c * 2 * step, 2 * step), 2 * step)

    def compute_y(c):
        value = multiply(c, x_high, x_low)

        @pl.when(at_end & (c >= CHUNKS - LATE))
        def _():
            partial[beside, rows(c)] = value

        high, low = split(value)
        base = pl.multiple_of(c * 2 * step, 2 * step)
        y_parts[pl.ds(base, step)] = high
        y_parts[pl.ds(pl.multiple_of(base + step, step), step)] = low

    def compute_square(c):
        square_ref[rows(c)] = multiply(c, a_high, a_low)

    def reduce_copy(right, d, c):
        target = jnp.where(right, z + 1, z - 1)
        slot = jnp.where(right & (d == target), n, d)
        return remote(
            partial.at[d, rows(c)], arrived.at[slot, rows(c)],
            reduce_send.at[d, c], reduce_recv.at[slot, c], col=target,
        )

    def reduce_wait(slot, c):
        remote(
            arrived.at[slot, rows(c)], arrived.at[slot, rows(c)],
            reduce_send.at[0, c], reduce_recv.at[slot, c], row=near,
        ).wait_recv()

    def compute_partial(c, d):
        block = pl.ds(pl.multiple_of(d * size, size), size)
        partial[d, rows(c)] = product(y_parts[y_rows(c)], a_high[block], a_low[block], transposed=True)

        @pl.when(((z == 0) & (d > 0)) | ((z == last) & (d < last)))
        def _():
            reduce_copy(z == 0, d, c).start()

    def pass_piece(d, c):
        reduce_wait(d, c)
        partial[d, rows(c)] = partial[d, rows(c)] + arrived[d, rows(c)]
        reduce_copy(d > z, d, c).start()

    def landed(piece):
        relay_wait(piece)
        if piece < 2:
            split_half((far, far_near)[piece], side)
            split_half((far_near, far)[piece], 1 - side)
        else:
            block = (far_outer, far_inner)[piece - 2]
            split_all(a_col.at[block], a_pair, block)
        if piece == 1:
            near_copy(0).wait_send()
            for sent_piece in range(2):
                far_copy(sent_piece).wait_send()
                relay_copy(sent_piece).wait_send()
        if piece == 3:
            for sent_piece in range(2, 4):
                far_copy(sent_piece).wait_send()
                relay_copy(sent_piece).wait_send()

            @pl.when(inside)
            def _():
                for at, row in ((0, near), (1, far)):
                    pl.semaphore_signal(
                        free_sems.at[at], inc=1, device_id={"row": row}, device_id_type=pl.DeviceIdType.MESH
                    )

    mirrored = z >= n // 2
    end_slot = jnp.where(mirrored, n - 2, 0)

    def end_copy(which):
        source, block, row = (
            (a_row.at[end_slot], r, far), (a_row.at[end_slot], r, near), (a_col.at[far], far, near)
        )[which]
        return remote(source, a_col.at[block], end_send.at[which], end_recv.at[which], row=row)

    def end_wait(which):
        block = (far, near, far_near)[which]
        remote(a_col.at[block], a_col.at[block], end_send.at[which], end_recv.at[which], row=near).wait_recv()

    def end_start():
        pl.semaphore_wait(free_sems.at[0], 1)
        pl.semaphore_wait(free_sems.at[1], 1)
        end_copy(0).start()
        end_copy(1).start()

    def end_middle():
        end_wait(0)
        end_copy(2).start()
        split_all(a_row.at[end_slot], x_pair, r)
        end_wait(1)
        split_all(a_col.at[near], x_pair, near)
        split_all(a_col.at[far], x_pair, far)

    def end_last():
        end_wait(2)
        split_all(a_col.at[far_near], x_pair, far_near)

    def end_partials(c):
        slot = jnp.where(mirrored, z, n)
        reduce_wait(slot, c)
        high, low = split(arrived[slot, rows(c)])
        lhs[:step, :size] = high
        lhs[step:, :size] = low

        def one(i):
            d = jnp.where(mirrored, i, last - i)
            block = pl.ds(pl.multiple_of(d * size, size), size)
            partial[d, rows(c)] = partial[d, rows(c)] + product(
                lhs[:, :size], x_high[block], x_low[block], transposed=True
            )

            @pl.when(i < n // 2)
            def _():
                reduce_copy(d > z, d, c).start()

        loop(0, n - 1, one)

    def facing(index):
        return jnp.where(mirrored, last - index, index)

    def other(index):
        return facing(jnp.where(index >= 1, index + 1, index))

    def act(code):
        def when(low, count, body):
            @pl.when((code >= low) & (code < low + count))
            def _():
                body((code - low) // CHUNKS, lax.rem(code - low, CHUNKS))

        def once(value, body):
            @pl.when(code == value)
            def _():
                body()

        when(0, 2 * CHUNKS, lambda i, c: gather_own((i == 0) != mirrored, c).start())
        when(16, 3 * CHUNKS, lambda i, c: pass_gather(other(i), c))
        when(40, 3 * CHUNKS, lambda i, c: pass_piece(other(i), c))

        def begin(i, c):
            gather_end(c)
            compute_y(c)

            @pl.when(at_end & (c >= CHUNKS - LATE))
            def _():
                reduce_copy(z == 0, beside, c).start()

        when(64, CHUNKS, begin)
        when(72, 4 * CHUNKS, lambda i, c: compute_partial(c, facing(i)))
        when(104, CHUNKS, lambda i, c: compute_square(c))
        for piece in range(4):
            once(112 + piece, functools.partial(relay, piece))
            once(116 + piece, functools.partial(landed, piece))
        once(120, lambda: split_both(x_col, x_pair))
        once(121, lambda: split_both(a_col, a_pair))
        once(122, end_start)
        once(123, end_middle)
        once(126, end_last)
        once(125, lambda: end_partials(CHUNKS - 1))

    def split_both(source, pair_refs):
        def one(i):
            block = jnp.where(i == 0, r, near)
            split_all(source.at[block], pair_refs, block)

        loop(0, 2, one)

    @pl.when(at_end)
    def _():
        loop(0, CHUNKS, own_both)

    @pl.when(inside)
    def _():
        loop(0, AHEAD, own_both)

    local[1].wait()
    far_copy(0).start()
    near_copy(0).start()
    local[0].wait()
    near_copy(1).start()
    local[2].start()
    near_wait(0)
    far_copy(1).start()
    near_wait(1)
    far_copy(2).start()
    far_copy(3).start()

    second = (pair == 0) == mirrored
    choice = jnp.where(at_end, 2, 0) + jnp.where(second, 1, 0)

    def four(i):
        word = 0
        for at in range(len(ORDERS[0])):
            value = ORDERS[3][at]
            for v in range(3):
                value = jnp.where(choice == v, ORDERS[v][at], value)
            word = jnp.where(i == at, value, word)

        def one(j, left):
            act(lax.rem(left, 128))
            return left // 128

        lax.fori_loop(0, 4, one, word)

    loop(0, len(ORDERS[0]), four)

    def finish(c):
        update_ref[rows(c)] = update_ref[rows(c)] + partial[z, rows(c)]

        early = c < CHUNKS - LATE

        @pl.when((z < last) & (early | (z != last - 1)))
        def _():
            reduce_wait(z, c)
            update_ref[rows(c)] = update_ref[rows(c)] + arrived[z, rows(c)]

        @pl.when((z > 0) & (early | (z != 1)))
        def _():
            reduce_wait(n, c)
            update_ref[rows(c)] = update_ref[rows(c)] + arrived[n, rows(c)]

    local[2].wait()
    loop(0, CHUNKS - 1, finish)

    near_copy(1).wait_send()

    @pl.when(inside)
    def _():
        for which in range(3):
            end_copy(which).wait_send()

    def sent(c):
        for hop in range(n - 1):
            @pl.when((z < last) & (z - hop >= 0))
            def _():
                gather_pass(True, z - hop, c).wait_send()

            @pl.when((z > 0) & (z + hop <= last))
            def _():
                gather_pass(False, z + hop, c).wait_send()

        for d in range(n):
            @pl.when((z != d) & (inside | (c < CHUNKS - LATE) | (d == beside)))
            def _():
                reduce_copy(z < d, d, c).wait_send()

    loop(0, CHUNKS, sent)
    finish(CHUNKS - 1)


def per_device(n, transition, covariance):
    size = transition.shape[0]
    f32, bf16 = jnp.float32, jnp.bfloat16
    return pl.pallas_call(
        functools.partial(kernel, n),
        out_shape=(pltpu.VMEM(transition.shape, f32),) * 2,
        in_specs=[pl.BlockSpec(memory_space=pl.ANY)] * 2,
        out_specs=(pl.BlockSpec(memory_space=pltpu.VMEM),) * 2,
        scratch_shapes=[
            pltpu.VMEM((n - 1, size, size), f32),
            pltpu.VMEM((n, size, size), f32),
            pltpu.VMEM((n, size, size), f32),
            pltpu.VMEM((n + 1, size, size), f32),
            pltpu.VMEM((n * size, size), bf16),
            pltpu.VMEM((n * size, size), bf16),
            pltpu.VMEM((n * size, size), bf16),
            pltpu.VMEM((n * size, size), bf16),
            pltpu.VMEM((2 * size, size), bf16),
            pltpu.VMEM((2 * size // CHUNKS, n * size), bf16),
            pltpu.SemaphoreType.DMA((3,)),
            pltpu.SemaphoreType.DMA((2,)),
            pltpu.SemaphoreType.DMA((2,)),
            pltpu.SemaphoreType.DMA((4,)),
            pltpu.SemaphoreType.DMA((4,)),
            pltpu.SemaphoreType.DMA((4,)),
            pltpu.SemaphoreType.DMA((4,)),
            pltpu.SemaphoreType.DMA((2, n - 1, CHUNKS)),
            pltpu.SemaphoreType.DMA((n - 1, CHUNKS)),
            pltpu.SemaphoreType.DMA((n, CHUNKS)),
            pltpu.SemaphoreType.DMA((n + 1, CHUNKS)),
            pltpu.SemaphoreType.DMA((3,)),
            pltpu.SemaphoreType.DMA((3,)),
            pltpu.SemaphoreType.REGULAR((2,)),
        ],
        compiler_params=pltpu.CompilerParams(
            collective_id=0, has_side_effects=True, vmem_limit_bytes=67043328 - 2 * 4 * transition.size
        ),
    )(transition, covariance)


def solution(mesh):
    n = mesh.shape["col"]
    assert mesh.shape["row"] == n == 4
    spec = P(("eq", "row"), "col")
    return jax.shard_map(
        functools.partial(per_device, n),
        mesh=mesh,
        in_specs=(spec, spec),
        out_specs=(spec, spec),
        check_vma=False,
    )
```

```python
import functools

import jax
import jax.numpy as jnp
from jax import lax
from jax.experimental import pallas as pl
from jax.experimental.pallas import tpu as pltpu
from jax.sharding import PartitionSpec as P

CHUNKS = 8
AHEAD = 2
LATE = 1
ORDERS = (
  (
    33733880, 36061464, 245106970, 6834592, 8964642, 44497649, 24142912, 156279941,
    158386980, 13052112, 173226308, 203262860, 79229281, 177533447, 119104157, 119761613,
    256490483, 190209368, 196546395, 197370683, 181640806, 149411879, 167368927, 106572687,
    108696681, 110826731, 129733997, 264952571, 95393391, 99456893,
  ),
  (
    33733880, 36061464, 245106970, 6834592, 8964642, 44497649, 24522816, 204890245,
    205886018, 13050330, 144485859, 152931212, 78832969, 160903687, 212950045, 100886237,
    120175603, 173303930, 147754835, 103001958, 181758542, 105373095, 167244743, 219536911,
    223138921, 227172075, 231560557, 265098747, 93020015, 99456893,
  ),
  (
    245120248, 137378545, 173302096, 141731016, 248703474, 209236192, 242430532, 190213239,
    162623067, 196699974, 221914086, 228046314, 234596973, 267757525, 268435455, 268435455,
    268435455, 268435455, 268435455, 268435455, 268435455, 268435455, 268435455, 268435455,
    268435455, 268435455, 268435455, 268435455, 268435455, 268435455,
  ),
  (
    245120248, 185613041, 188244192, 141996354, 248967666, 158508232, 161033796, 146029555,
    213165777, 175353542, 221914086, 228257642, 180074196, 267757551, 268435455, 268435455,
    268435455, 268435455, 268435455, 268435455, 268435455, 268435455, 268435455, 268435455,
    268435455, 268435455, 268435455, 268435455, 268435455, 268435455,
  ),
)


def split(value):
    high = value.astype(jnp.bfloat16)
    return high, (value - high.astype(jnp.float32)).astype(jnp.bfloat16)


def product(stacked, high, low, transposed=False):
    dims = (((1,), (1 if transposed else 0,)), ((), ()))
    dot = functools.partial(lax.dot_general, dimension_numbers=dims, preferred_element_type=jnp.float32)
    step = stacked.shape[0] // 2
    both = dot(stacked, high)
    return both[:step] + (both[step:] + dot(stacked[:step], low))


def kernel(
    n, a_ref, x_ref, update_ref, square_ref,
    a_row, a_col, x_col, arrived, x_high, x_low, a_high, a_low, y_parts, lhs,
    local_sems, near_send, near_recv, far_send, far_recv, relay_send, relay_recv,
    gather_send, gather_recv, reduce_send, reduce_recv, end_send, end_recv, free_sems,
):
    r, z = lax.axis_index("row"), lax.axis_index("col")
    size = a_ref.shape[0]
    step = size // CHUNKS
    half_rows = size // 2
    last = n - 1
    pair = r // 2
    side = lax.rem(r, 2)
    far = lax.rem(r + n // 2, n)
    near = r + 1 - 2 * side
    far_near = lax.rem(near + n // 2, n)
    own_outer = jnp.where(pair == 0, 0, last)
    own_inner = jnp.where(pair == 0, 1, last - 1)
    far_outer = last - own_outer
    far_inner = last - own_inner
    at_end = (z == 0) | (z == last)
    inside = (z > 0) & (z < last)
    beside = jnp.where(z == 0, 1, last - 1)

    def rows(c):
        return pl.ds(pl.multiple_of(c * step, step), step)

    def loop(low, high, body):
        def one(i, carry):
            body(i)
            return carry

        lax.fori_loop(low, high, one, 0)

    def remote(src, dst, send, recv, **where):
        return pltpu.make_async_remote_copy(
            src_ref=src, dst_ref=dst, send_sem=send, recv_sem=recv,
            device_id=where, device_id_type=pl.DeviceIdType.MESH,
        )

    partial = x_col
    local = [
        pltpu.make_async_copy(a_ref, a_col.at[r], local_sems.at[0]),
        pltpu.make_async_copy(x_ref, x_col.at[r], local_sems.at[1]),
        pltpu.make_async_copy(x_ref, update_ref, local_sems.at[2]),
    ]
    for copy in local[:2]:
        copy.start()

    barrier = pltpu.get_barrier_semaphore()

    def greet(**where):
        pl.semaphore_signal(barrier, inc=1, device_id=where, device_id_type=pl.DeviceIdType.MESH)

    greet(row=far)
    greet(row=near)

    @pl.when(z > 0)
    def _():
        greet(col=z - 1)

    @pl.when(z < last)
    def _():
        greet(col=z + 1)

    pl.semaphore_wait(barrier, 4 - jnp.where(z == 0, 1, 0) - jnp.where(z == last, 1, 0))

    def gather_copy(right, block, c):
        slot = jnp.where(right, block, block - 1)
        landing = a_row.at[slot, rows(c)]
        sems = gather_send.at[jnp.where(right, 0, 1), jnp.abs(block - z), c], gather_recv.at[slot, c]
        to = jnp.where(right, z + 1, z - 1)
        return landing, sems, to

    def gather_own(right, c):
        landing, sems, to = gather_copy(right, z, c)
        return remote(a_ref.at[rows(c)], landing, *sems, col=to)

    def gather_pass(right, block, c):
        landing, sems, to = gather_copy(right, block, c)
        return remote(landing, landing, *sems, col=to)

    def gather_arrival(block, c):
        slot = jnp.where(block > z, block - 1, block)
        remote(
            a_row.at[slot, rows(c)], a_row.at[slot, rows(c)],
            gather_send.at[0, 0, c], gather_recv.at[slot, c], row=near,
        ).wait_recv()

    def own_both(c):
        @pl.when(z < last)
        def _():
            gather_own(True, c).start()

        @pl.when(z > 0)
        def _():
            gather_own(False, c).start()

    def pass_gather(block, c):
        gather_arrival(block, c)
        gather_pass(block < z, block, c).start()

    def gather_end(c):
        @pl.when(at_end)
        def _():
            for hop in range(1, n):
                gather_arrival(jnp.where(z == 0, hop, last - hop), c)

    def near_copy(which):
        buffer = (x_col, a_col)[which]
        return remote(buffer.at[r], buffer.at[r], near_send.at[which], near_recv.at[which], row=near)

    def near_wait(which):
        buffer = (x_col, a_col)[which]
        remote(buffer.at[near], buffer.at[near], near_send.at[which], near_recv.at[which], row=near).wait_recv()

    def half_of(piece, mine, rows_of):
        buffer = x_col if piece < 2 else a_col
        if piece < 2:
            block = (r, near)[piece] if mine else (far, far_near)[piece]
        else:
            block = ((own_outer, own_inner) if mine else (far_outer, far_inner))[piece - 2]
        return buffer.at[block, pl.ds(pl.multiple_of(rows_of * half_rows, half_rows), half_rows)]

    def far_copy(piece):
        ref = half_of(piece, True, side)
        return remote(ref, ref, far_send.at[piece], far_recv.at[piece], row=far)

    def relay_copy(piece):
        ref = half_of(piece, False, side)
        return remote(ref, ref, relay_send.at[piece], relay_recv.at[piece], row=near)

    def relay(piece):
        ref = half_of(piece, False, side)
        remote(ref, ref, far_send.at[piece], far_recv.at[piece], row=far).wait_recv()
        relay_copy(piece).start()

    def relay_wait(piece):
        ref = half_of(piece, False, 1 - side)
        remote(ref, ref, relay_send.at[piece], relay_recv.at[piece], row=near).wait_recv()

    x_pair, a_pair = (x_high, x_low), (a_high, a_low)

    def split_rows(source, pair_refs, block, low_row, count):
        def some(i):
            at = pl.multiple_of(low_row + i * step, step)
            to = pl.ds(pl.multiple_of(block * size + at, step), step)
            pair_refs[0][to], pair_refs[1][to] = split(source[pl.ds(at, step)])

        loop(0, count // step, some)

    def split_half(block, which_half):
        split_rows(x_col.at[block], x_pair, block, which_half * half_rows, half_rows)

    def split_all(source, pair_refs, block):
        split_rows(source, pair_refs, block, 0, size)

    def multiply(c, high_ref, low_ref):
        for hop in range(n):
            block = lax.rem(z + hop, n)
            slot = jnp.where(block > z, block - 1, block)
            high, low = split(a_col[r, rows(c)] if hop == 0 else a_row[slot, rows(c)])
            to = pl.ds(pl.multiple_of(block * size, size), size)
            lhs[:step, to] = high
            lhs[step:, to] = low
        return product(lhs[...], high_ref[...], low_ref[...])

    def y_rows(c):
        return pl.ds(pl.multiple_of(c * 2 * step, 2 * step), 2 * step)

    def compute_y(c):
        value = multiply(c, x_high, x_low)

        @pl.when(at_end & (c >= CHUNKS - LATE))
        def _():
            partial[beside, rows(c)] = value

        high, low = split(value)
        base = pl.multiple_of(c * 2 * step, 2 * step)
        y_parts[pl.ds(base, step)] = high
        y_parts[pl.ds(pl.multiple_of(base + step, step), step)] = low

    def compute_square(c):
        square_ref[rows(c)] = multiply(c, a_high, a_low)

    def reduce_copy(right, d, c):
        target = jnp.where(right, z + 1, z - 1)
        slot = jnp.where(right & (d == target), n, d)
        return remote(
            partial.at[d, rows(c)], arrived.at[slot, rows(c)],
            reduce_send.at[d, c], reduce_recv.at[slot, c], col=target,
        )

    def reduce_wait(slot, c):
        remote(
            arrived.at[slot, rows(c)], arrived.at[slot, rows(c)],
            reduce_send.at[0, c], reduce_recv.at[slot, c], row=near,
        ).wait_recv()

    def compute_partial(c, d):
        block = pl.ds(pl.multiple_of(d * size, size), size)
        partial[d, rows(c)] = product(y_parts[y_rows(c)], a_high[block], a_low[block], transposed=True)

        @pl.when(((z == 0) & (d > 0)) | ((z == last) & (d < last)))
        def _():
            reduce_copy(z == 0, d, c).start()

    def pass_piece(d, c):
        reduce_wait(d, c)
        partial[d, rows(c)] = partial[d, rows(c)] + arrived[d, rows(c)]
        reduce_copy(d > z, d, c).start()

    def landed(piece):
        relay_wait(piece)
        if piece < 2:
            split_half((far, far_near)[piece], side)
            split_half((far_near, far)[piece], 1 - side)
        else:
            block = (far_outer, far_inner)[piece - 2]
            split_all(a_col.at[block], a_pair, block)
        if piece == 1:
            near_copy(0).wait_send()
            for sent_piece in range(2):
                far_copy(sent_piece).wait_send()
                relay_copy(sent_piece).wait_send()
        if piece == 3:
            for sent_piece in range(2, 4):
                far_copy(sent_piece).wait_send()
                relay_copy(sent_piece).wait_send()

            @pl.when(inside)
            def _():
                for at, row in ((0, near), (1, far)):
                    pl.semaphore_signal(
                        free_sems.at[at], inc=1, device_id={"row": row}, device_id_type=pl.DeviceIdType.MESH
                    )

    mirrored = z >= n // 2
    end_slot = jnp.where(mirrored, n - 2, 0)

    def end_copy(which):
        source, block, row = (
            (a_row.at[end_slot], r, far), (a_row.at[end_slot], r, near), (a_col.at[far], far, near)
        )[which]
        return remote(source, a_col.at[block], end_send.at[which], end_recv.at[which], row=row)

    def end_wait(which):
        block = (far, near, far_near)[which]
        remote(a_col.at[block], a_col.at[block], end_send.at[which], end_recv.at[which], row=near).wait_recv()

    def end_start():
        pl.semaphore_wait(free_sems.at[0], 1)
        pl.semaphore_wait(free_sems.at[1], 1)
        end_copy(0).start()
        end_copy(1).start()

    def end_middle():
        end_wait(0)
        end_copy(2).start()
        split_all(a_row.at[end_slot], x_pair, r)
        end_wait(1)
        split_all(a_col.at[near], x_pair, near)
        split_all(a_col.at[far], x_pair, far)

    def end_last():
        end_wait(2)
        split_all(a_col.at[far_near], x_pair, far_near)

    def end_partials(c):
        slot = jnp.where(mirrored, z, n)
        reduce_wait(slot, c)
        high, low = split(arrived[slot, rows(c)])
        lhs[:step, :size] = high
        lhs[step:, :size] = low

        def one(i):
            d = jnp.where(mirrored, i, last - i)
            block = pl.ds(pl.multiple_of(d * size, size), size)
            partial[d, rows(c)] = partial[d, rows(c)] + product(
                lhs[:, :size], x_high[block], x_low[block], transposed=True
            )

            @pl.when(i < n // 2)
            def _():
                reduce_copy(d > z, d, c).start()

        loop(0, n - 1, one)

    def facing(index):
        return jnp.where(mirrored, last - index, index)

    def other(index):
        return facing(jnp.where(index >= 1, index + 1, index))

    def act(code):
        def when(low, count, body):
            @pl.when((code >= low) & (code < low + count))
            def _():
                body((code - low) // CHUNKS, lax.rem(code - low, CHUNKS))

        def once(value, body):
            @pl.when(code == value)
            def _():
                body()

        when(0, 2 * CHUNKS, lambda i, c: gather_own((i == 0) != mirrored, c).start())
        when(16, 3 * CHUNKS, lambda i, c: pass_gather(other(i), c))
        when(40, 3 * CHUNKS, lambda i, c: pass_piece(other(i), c))

        def begin(i, c):
            gather_end(c)
            compute_y(c)

            @pl.when(at_end & (c >= CHUNKS - LATE))
            def _():
                reduce_copy(z == 0, beside, c).start()

        when(64, CHUNKS, begin)
        when(72, 4 * CHUNKS, lambda i, c: compute_partial(c, facing(i)))
        when(104, CHUNKS, lambda i, c: compute_square(c))
        for piece in range(4):
            once(112 + piece, functools.partial(relay, piece))
            once(116 + piece, functools.partial(landed, piece))
        once(120, lambda: split_both(x_col, x_pair))
        once(121, lambda: split_both(a_col, a_pair))
        once(122, end_start)
        once(123, end_middle)
        once(126, end_last)
        once(125, lambda: end_partials(CHUNKS - 1))

    def split_both(source, pair_refs):
        def one(i):
            block = jnp.where(i == 0, r, near)
            split_all(source.at[block], pair_refs, block)

        loop(0, 2, one)

    @pl.when(at_end)
    def _():
        loop(0, CHUNKS, own_both)

    @pl.when(inside)
    def _():
        loop(0, AHEAD, own_both)

    local[1].wait()
    far_copy(0).start()
    near_copy(0).start()
    local[0].wait()
    near_copy(1).start()
    local[2].start()
    near_wait(0)
    far_copy(1).start()
    near_wait(1)
    far_copy(2).start()
    far_copy(3).start()

    second = (pair == 0) == mirrored
    choice = jnp.where(at_end, 2, 0) + jnp.where(second, 1, 0)

    def four(i):
        word = 0
        for at in range(len(ORDERS[0])):
            value = ORDERS[3][at]
            for v in range(3):
                value = jnp.where(choice == v, ORDERS[v][at], value)
            word = jnp.where(i == at, value, word)

        def one(j, left):
            act(lax.rem(left, 128))
            return left // 128

        lax.fori_loop(0, 4, one, word)

    loop(0, len(ORDERS[0]), four)

    def finish(c):
        update_ref[rows(c)] = update_ref[rows(c)] + partial[z, rows(c)]

        early = c < CHUNKS - LATE

        @pl.when((z < last) & (early | (z != last - 1)))
        def _():
            reduce_wait(z, c)
            update_ref[rows(c)] = update_ref[rows(c)] + arrived[z, rows(c)]

        @pl.when((z > 0) & (early | (z != 1)))
        def _():
            reduce_wait(n, c)
            update_ref[rows(c)] = update_ref[rows(c)] + arrived[n, rows(c)]

    local[2].wait()
    loop(0, CHUNKS - 1, finish)

    near_copy(1).wait_send()

    @pl.when(inside)
    def _():
        for which in range(3):
            end_copy(which).wait_send()

    def sent(c):
        for hop in range(n - 1):
            @pl.when((z < last) & (z - hop >= 0))
            def _():
                gather_pass(True, z - hop, c).wait_send()

            @pl.when((z > 0) & (z + hop <= last))
            def _():
                gather_pass(False, z + hop, c).wait_send()

        for d in range(n):
            @pl.when((z != d) & (inside | (c < CHUNKS - LATE) | (d == beside)))
            def _():
                reduce_copy(z < d, d, c).wait_send()

    loop(0, CHUNKS, sent)
    finish(CHUNKS - 1)


def store(update_ref, square_ref, update_out, square_out, sems):
    copies = [
        pltpu.make_async_copy(update_ref, update_out, sems.at[0]),
        pltpu.make_async_copy(square_ref, square_out, sems.at[1]),
    ]
    for copy in copies:
        copy.start()
    for copy in copies:
        copy.wait()


def per_device(n, transition, covariance):
    size = transition.shape[0]
    f32, bf16 = jnp.float32, jnp.bfloat16
    update, square = pl.pallas_call(
        functools.partial(kernel, n),
        out_shape=(pltpu.VMEM(transition.shape, f32),) * 2,
        in_specs=[pl.BlockSpec(memory_space=pl.ANY)] * 2,
        out_specs=(pl.BlockSpec(memory_space=pltpu.VMEM),) * 2,
        scratch_shapes=[
            pltpu.VMEM((n - 1, size, size), f32),
            pltpu.VMEM((n, size, size), f32),
            pltpu.VMEM((n, size, size), f32),
            pltpu.VMEM((n + 1, size, size), f32),
            pltpu.VMEM((n * size, size), bf16),
            pltpu.VMEM((n * size, size), bf16),
            pltpu.VMEM((n * size, size), bf16),
            pltpu.VMEM((n * size, size), bf16),
            pltpu.VMEM((2 * size, size), bf16),
            pltpu.VMEM((2 * size // CHUNKS, n * size), bf16),
            pltpu.SemaphoreType.DMA((3,)),
            pltpu.SemaphoreType.DMA((2,)),
            pltpu.SemaphoreType.DMA((2,)),
            pltpu.SemaphoreType.DMA((4,)),
            pltpu.SemaphoreType.DMA((4,)),
            pltpu.SemaphoreType.DMA((4,)),
            pltpu.SemaphoreType.DMA((4,)),
            pltpu.SemaphoreType.DMA((2, n - 1, CHUNKS)),
            pltpu.SemaphoreType.DMA((n - 1, CHUNKS)),
            pltpu.SemaphoreType.DMA((n, CHUNKS)),
            pltpu.SemaphoreType.DMA((n + 1, CHUNKS)),
            pltpu.SemaphoreType.DMA((3,)),
            pltpu.SemaphoreType.DMA((3,)),
            pltpu.SemaphoreType.REGULAR((2,)),
        ],
        compiler_params=pltpu.CompilerParams(
            collective_id=0, has_side_effects=True, vmem_limit_bytes=67043328 - 2 * 4 * transition.size
        ),
    )(transition, covariance)
    shape = jax.ShapeDtypeStruct(transition.shape, f32)
    return pl.pallas_call(
        store,
        out_shape=(shape, shape),
        in_specs=[pl.BlockSpec(memory_space=pl.ANY)] * 2,
        out_specs=(pl.BlockSpec(memory_space=pl.ANY),) * 2,
        scratch_shapes=[pltpu.SemaphoreType.DMA((2,))],
        compiler_params=pltpu.CompilerParams(vmem_limit_bytes=1 << 20),
    )(update, square)


def solution(mesh):
    n = mesh.shape["col"]
    assert mesh.shape["row"] == n == 4
    spec = P(("eq", "row"), "col")
    return jax.shard_map(
        functools.partial(per_device, n),
        mesh=mesh,
        in_specs=(spec, spec),
        out_specs=(spec, spec),
        check_vma=False,
    )
```
